32 devices in a mesh: lon: 8 (over z, core), colat: 4 (over y, x).
Axes of the slice: x: 2, y: 2, z: 4, core: 2. Of those that a mesh axis runs over, the one named last changes fastest.
Arguments:
- forward_state: float32 [9, 8, 64, 1024], P(None, None, 'colat', 'lon'), may hold values from -6 to 6
- adjoint_state: float32 [9, 8, 64, 1024], P(None, None, 'colat', 'lon'), may hold values from -6 to 6
- layer_ids: int32 [8, 64, 1024], P(None, 'colat', 'lon'), may hold values from 0 to 15
- density_table: float32 [16], replicated, may hold values from 2 to 4
- lame_table: float32 [16], replicated, may hold values from 0.5 to 2
- shear_table: float32 [16], replicated, may hold values from 0.5 to 1.5
- source_cells: int32 [8], replicated, may hold values from 0 to 524287
- source_wavelet: float32 [2, 8], replicated, may hold values from -6 to 6
- receiver_cells: int32 [512], replicated, may hold values from 0 to 524287
- receiver_residual: float32 [2, 3, 512], replicated, may hold values from -6 to 6
Outputs:
- forward_field: float32 [9, 8, 64, 1024], P(None, None, 'colat', 'lon')
- adjoint_field: float32 [9, 8, 64, 1024], P(None, None, 'colat', 'lon')
- density_kernel: float32 [8, 64, 1024], P(None, 'colat', 'lon')
The draws below stay inside these ranges and needn't reach their ends.
Inputs may be any that keep to these rules, and one draw needn't show every extreme that they name: `source_cells`: flat index (level * 64 + colatitude) * 1024 + longitude. `receiver_cells`: flat index as for the sources.
All inputs are finite; a program needn't handle non-finite values.
Results may differ from the reference program's by a relative error of at most 0.0001.
Values sent between devices are 32-bit elements; how exact they have to be, the bound alone decides.
No kernel may reach another device: no remote copies, remote signals or barrier semaphores. Data moves between devices by JAX's collectives and lax.ppermute only.
A program may use at most 64 MiB of HBM per device.

```python
import math
import jax
import jax.numpy as jnp

R = 8
STEPS = 2
NLAYER = 16
NSRC = 8
NREC = 512
NTH = 64
NPH = 1024


def place_ends(values, stream_key, low, high):
    dims = values.shape
    place = [jax.random.randint(jax.random.fold_in(stream_key, axis), (), 0, dims[axis]) for axis in range(len(dims))]
    values = values.at[tuple(place)].set(low)
    longest = dims.index(max(dims))
    place[longest] = (place[longest] + 1) % dims[longest]
    return values.at[tuple(place)].set(high)


def steps_of(own_key, dims, pieces, low, largest):
    factor_of, own = 1.0, jax.random.fold_in(own_key, 6)
    for dim, blocks in pieces:
        draws = jnp.exp(jax.random.uniform(jax.random.fold_in(own, dim), (blocks,), jnp.float32, low / len(pieces), largest / len(pieces)))
        factor_of = factor_of * jnp.repeat(draws, dims[dim] // blocks).reshape([-1 if axis == dim else 1 for axis in range(len(dims))])
    return factor_of


def scatter_about(key, dims, deviation, reach, cuts=(), kind=jnp.bfloat16):
    result = deviation * jax.random.normal(key, dims, jnp.float32)
    if cuts:
        result = result * steps_of(key, dims, cuts, -0.22, 0.18)
    return jnp.clip(result, -reach, reach).astype(kind)


def setup_inputs(seed: int = 0) -> dict:
    streams_of = jax.random.split(jax.random.key(seed), 11)
    forward_state = scatter_about(streams_of[0], (9, R, NTH, NPH), 1.0, 6.0, ((2, 4), (3, 8)), jnp.float32)
    adjoint_state = scatter_about(streams_of[1], (9, R, NTH, NPH), 1.0, 6.0, ((2, 4), (3, 8)), jnp.float32)
    layer_ids = place_ends(jax.random.randint(streams_of[2], (R, NTH, NPH), 0, NLAYER), jax.random.fold_in(streams_of[2], 1), 0, NLAYER - 1).astype(jnp.int32)
    density_table = jnp.clip(jax.random.uniform(streams_of[3], (NLAYER,), jnp.float32, 2.0, 4.0), 2.0, 4.0)
    lame_table = jnp.clip(jax.random.uniform(streams_of[4], (NLAYER,), jnp.float32, 0.5, 2.0), 0.5, 2.0)
    shear_table = jnp.clip(jax.random.uniform(streams_of[5], (NLAYER,), jnp.float32, 0.5, 1.5), 0.5, 1.5)
    source_cells = place_ends(jax.random.randint(streams_of[6], (NSRC,), 0, R * NTH * NPH), jax.random.fold_in(streams_of[6], 1), 0, (R * NTH * NPH) - 1).astype(jnp.int32)
    source_wavelet = scatter_about(streams_of[7], (STEPS, NSRC), 1.0, 6.0, (), jnp.float32)
    receiver_cells = place_ends(jax.random.randint(streams_of[8], (NREC,), 0, R * NTH * NPH), jax.random.fold_in(streams_of[8], 1), 0, (R * NTH * NPH) - 1).astype(jnp.int32)
    receiver_residual = scatter_about(streams_of[9], (STEPS, 3, NREC), 1.0, 6.0, (), jnp.float32)
    return dict(forward_state=forward_state, adjoint_state=adjoint_state, layer_ids=layer_ids, density_table=density_table, lame_table=lame_table, shear_table=shear_table, source_cells=source_cells, source_wavelet=source_wavelet, receiver_cells=receiver_cells, receiver_residual=receiver_residual)


R_INNER = 0.55
COURANT = 0.3
SIN_FLOOR = 0.25
VEL_SIGNS = (-1.0, -1.0, 1.0)
STRESS_SIGNS = (1.0, 1.0, 1.0, 1.0, -1.0, -1.0)


def geometry(row_ids, levels, lat_cells, lon_cells):
    theta_step = math.pi / lat_cells
    phi_step = 2.0 * math.pi / lon_cells
    delta_r = (1.0 - R_INNER) / levels
    radius = R_INNER + (jnp.arange(levels, dtype=jnp.float32) + 0.5) * delta_r
    colatitude = (row_ids.astype(jnp.float32) + 0.5) * theta_step
    sines_held = jnp.maximum(jnp.sin(colatitude), SIN_FLOOR)
    cotangent = jnp.cos(colatitude) / sines_held
    inv_radius = (1.0 / radius)[:, None, None]
    along_theta = inv_radius / theta_step
    along_phi = inv_radius / (sines_held[None, :, None] * phi_step)
    curvature = cotangent[None, :, None] * inv_radius
    return along_theta, along_phi, curvature, inv_radius, 1.0 / delta_r


def time_step(lon_cells):
    return COURANT * SIN_FLOOR * R_INNER * (2.0 * math.pi / lon_cells) / 1.6


def diff_theta(values):
    return (8.0 * (values[..., 3:-1, 2:-2] - values[..., 1:-3, 2:-2]) - (values[..., 4:, 2:-2] - values[..., :-4, 2:-2])) / 12.0


def diff_phi(values):
    return (8.0 * (values[..., 2:-2, 3:-1] - values[..., 2:-2, 1:-3]) - (values[..., 2:-2, 4:] - values[..., 2:-2, :-4])) / 12.0


def diff_radial(values):
    padded = jnp.pad(values, [(0, 0)] * (values.ndim - 3) + [(1, 1), (0, 0), (0, 0)])
    return (padded[..., 2:, :, :] - padded[..., :-2, :, :]) * 0.5


def accelerate(stress, metric):
    along_theta, along_phi, curvature, inv_radius, inv_spacing = metric
    centre_part = stress[..., 2:-2, 2:-2]
    stress_tt, stress_pp, stress_rr = centre_part[:, 0], centre_part[:, 1], centre_part[:, 2]
    stress_tp, stress_tr, stress_pr = centre_part[:, 3], centre_part[:, 4], centre_part[:, 5]
    theta_diff = diff_theta(stress)
    phi_diff = diff_phi(stress)
    radial_diff = diff_radial(centre_part)
    force_theta = along_theta * theta_diff[:, 0] + along_phi * phi_diff[:, 3] + inv_spacing * radial_diff[:, 4] + curvature * (stress_tt - stress_pp) + 3.0 * inv_radius * stress_tr
    force_phi = along_theta * theta_diff[:, 3] + along_phi * phi_diff[:, 1] + inv_spacing * radial_diff[:, 5] + 2.0 * curvature * stress_tp + 3.0 * inv_radius * stress_pr
    force_radial = along_theta * theta_diff[:, 4] + along_phi * phi_diff[:, 5] + inv_spacing * radial_diff[:, 2] + inv_radius * (2.0 * stress_rr - stress_tt - stress_pp) + curvature * stress_tr
    return jnp.stack([force_theta, force_phi, force_radial], 1)


def stress_rate(velocity, lame_field, shear_field, metric):
    along_theta, along_phi, curvature, inv_radius, inv_spacing = metric
    centre_part = velocity[..., 2:-2, 2:-2]
    vel_theta, vel_phi, vel_radial = centre_part[:, 0], centre_part[:, 1], centre_part[:, 2]
    theta_diff = diff_theta(velocity)
    phi_diff = diff_phi(velocity)
    radial_diff = diff_radial(centre_part)
    strain_tt = along_theta * theta_diff[:, 0] + inv_radius * vel_radial
    strain_pp = along_phi * phi_diff[:, 1] + curvature * vel_theta + inv_radius * vel_radial
    strain_rr = inv_spacing * radial_diff[:, 2]
    strain_tp = 0.5 * (along_theta * theta_diff[:, 1] - curvature * vel_phi + along_phi * phi_diff[:, 0])
    strain_tr = 0.5 * (inv_spacing * radial_diff[:, 0] - inv_radius * vel_theta + along_theta * theta_diff[:, 2])
    strain_pr = 0.5 * (inv_spacing * radial_diff[:, 1] - inv_radius * vel_phi + along_phi * phi_diff[:, 2])
    dilation = strain_tt + strain_pp + strain_rr
    double_shear = 2.0 * shear_field
    return jnp.stack([lame_field * dilation + double_shear * strain_tt, lame_field * dilation + double_shear * strain_pp,
                      lame_field * dilation + double_shear * strain_rr, double_shear * strain_tp,
                      double_shear * strain_tr, double_shear * strain_pr], 1)


def fold_rows(fields, rim_width, sign_flip):
    half_turn = fields.shape[-1] // 2
    upper_strip = jnp.roll(fields[..., :rim_width, :][..., ::-1, :], half_turn, axis=-1) * sign_flip
    lower_strip = jnp.roll(fields[..., -rim_width:, :][..., ::-1, :], half_turn, axis=-1) * sign_flip
    fields = jnp.concatenate([upper_strip, fields, lower_strip], -2)
    return jnp.concatenate([fields[..., -rim_width:], fields, fields[..., :rim_width]], -1)


def reference(forward_state, adjoint_state, layer_ids, density_table, lame_table, shear_table, source_cells, source_wavelet, receiver_cells, receiver_residual):
    levels, lat_cells, lon_cells = layer_ids.shape
    metric = geometry(jnp.arange(lat_cells, dtype=jnp.int32), levels, lat_cells, lon_cells)
    step_size = time_step(lon_cells)
    inv_rho = 1.0 / density_table[layer_ids]
    lame_field = lame_table[layer_ids]
    shear_field = shear_table[layer_ids]
    vel_flip = jnp.array(VEL_SIGNS, dtype=jnp.float32)[:, None, None, None]
    stress_flip = jnp.array(STRESS_SIGNS, dtype=jnp.float32)[:, None, None, None]
    stacked = jnp.stack([forward_state, adjoint_state])
    velocity = stacked[:, :3]
    stress = stacked[:, 3:]
    plane_cells = lat_cells * lon_cells
    source_level = source_cells // plane_cells
    source_row = (source_cells % plane_cells) // lon_cells
    source_col = source_cells % lon_cells
    receiver_level = receiver_cells // plane_cells
    receiver_row = (receiver_cells % plane_cells) // lon_cells
    receiver_col = receiver_cells % lon_cells
    kernel = jnp.zeros(layer_ids.shape, jnp.float32)
    for step_index in range(STEPS):
        forcing = accelerate(fold_rows(stress, 2, stress_flip), metric)
        velocity = velocity + step_size * inv_rho * forcing
        velocity = velocity.at[0, 2, source_level, source_row, source_col].add(source_wavelet[step_index])
        for component in range(3):
            velocity = velocity.at[1, component, receiver_level, receiver_row, receiver_col].add(receiver_residual[step_index, component])
        stress = stress + step_size * stress_rate(fold_rows(velocity, 2, vel_flip), lame_field, shear_field, metric)
        kernel = kernel + jnp.sum(velocity[0] * velocity[1], 0)
    forward_field = jnp.concatenate([velocity[0], stress[0]], 0)
    adjoint_field = jnp.concatenate([velocity[1], stress[1]], 0)
    return forward_field, adjoint_field, kernel
```

```python
import functools
import math

import jax
import jax.numpy as jnp
from jax import lax
from jax.experimental import pallas as pl
from jax.experimental.pallas import tpu as pltpu
from jax.sharding import PartitionSpec as P

STEPS = 2
R_INNER = 0.55
COURANT = 0.3
SIN_FLOOR = 0.25
FIELD_SIGNS = (-1, -1, 1, 1, 1, 1, 1, -1, -1)
CROSS = (3, 6, 7)
OTHER = (4, 5, 8)
EDGE = 8
LANES = 128
V_ROWS = 6
S_ROWS = 4
F32 = jnp.float32


NEAR = tuple((f, c, d) for f in range(2) for c in CROSS for d in (1, 2))
FAR = tuple((f, c, d) for f in range(2) for c in OTHER for d in (1, 2)) + tuple(
    (f, c, d) for f in range(2) for c in CROSS for d in (3, 4)
)
FAR_IDS = len(FAR)
VEL = tuple((f, c, d) for f in range(2) for c in range(3) for d in range(1, V_ROWS + 1))


def vmem():
    return pl.BlockSpec(memory_space=pltpu.VMEM)


def smem():
    return pl.BlockSpec(memory_space=pltpu.SMEM)


def lane_iota(shape):
    return lax.broadcasted_iota(jnp.int32, shape, 1)


def rolled(x, shift, axis=1):
    size = x.shape[axis]
    shift = shift % size
    return x if shift == 0 else pltpu.roll(x, shift, axis)


class Packer:
    def __init__(self, ref, width, base=0):
        self.ref, self.width, self.base = ref, width, base
        self.per = LANES // width
        self.count, self.value = 0, None

    def add(self, x, start):
        slot = self.count % self.per
        moved = rolled(x, slot * self.width - start)
        if slot == 0:
            self.value = moved
        else:
            self.value = jnp.where(lane_iota(x.shape) >= slot * self.width, moved, self.value)
        self.count += 1
        if self.count % self.per == 0:
            self.flush()

    def flush(self):
        if self.value is not None:
            self.ref[self.base + (self.count - 1) // self.per] = self.value
            self.value = None


def pieces(count, width):
    per = LANES // width
    return -(-count // per)


def unpack_edges(east_ref, west_ref, j):
    per = LANES // EDGE
    v, slot = j // per, j % per
    return halo_vector(east_ref[v], west_ref[v], slot)


def halo_vector(east, west, slot):
    after = rolled(east, -slot * EDGE)
    before = rolled(west, LANES - EDGE - slot * EDGE)
    return jnp.where(lane_iota(after.shape) < LANES // 2, after, before)


def facing():
    lon, half = lax.axis_index("lon"), lax.axis_size("lon") // 2
    count = lax.axis_size("lon")
    here = lon < half
    to_west = lax.rem(lon + count - 1, count) < half
    to_east = lax.rem(lon + 1, count) < half
    return here, to_west, to_east


def pole_signs():
    band, last = lax.axis_index("colat"), lax.axis_size("colat") - 1
    north = jnp.where(band == 0, -1.0, 1.0).astype(F32)
    south = jnp.where(band == last, -1.0, 1.0).astype(F32)
    return north, south


def strided(ref, first, levels, rows):
    return ref[pl.ds(first, levels, stride=rows), :]


def pack_kernel(
    dims, fwd, adj, ids, east, west, near_f, near_b, far_f, far_b, d_ef, d_eb, d_wf, d_wb
):
    levels, rows, cols = dims
    here, _, _ = facing()

    def row(f, c, r):
        return strided((fwd, adj)[f], c * levels * rows + r, levels, rows)

    def id_row(r):
        return strided(ids, r, levels, rows).astype(F32)

    def facing_rows(get, d):
        top, bottom = get(d - 1), get(rows - d)
        return jnp.where(here, bottom, top), jnp.where(here, top, bottom)

    diag = [Packer(ref, EDGE) for ref in (d_ef, d_eb, d_wf, d_wb)]

    def put(ref_f, ref_b, k, get, d):
        f, b = facing_rows(get, d)
        ref_f[k], ref_b[k] = f, b
        diag[0].add(f[:, cols - LANES :], LANES - EDGE)
        diag[1].add(b[:, cols - LANES :], LANES - EDGE)
        diag[2].add(f[:, :LANES], 0)
        diag[3].add(b[:, :LANES], 0)

    for k, (f, c, d) in enumerate(NEAR):
        put(near_f, near_b, k, functools.partial(row, f, c), d)
    for k, (f, c, d) in enumerate(FAR):
        put(far_f, far_b, k, functools.partial(row, f, c), d)
    for d in range(1, S_ROWS + 1):
        put(far_f, far_b, FAR_IDS + d - 1, id_row, d)
    for packer in diag:
        packer.flush()

    packs = Packer(east, EDGE), Packer(west, EDGE)

    def both(x):
        packs[0].add(x[:, cols - LANES :], LANES - EDGE)
        packs[1].add(x[:, :LANES], 0)

    for f in range(2):
        for c in range(9):
            for r in range(rows):
                both(row(f, c, r))
    for r in range(rows):
        both(id_row(r))
    for packer in packs:
        packer.flush()


def inject_kernel(dims, cells, values, scells, svalues, first, second):
    levels, rows, cols = dims
    width = cols + LANES
    north_sign, south_sign = pole_signs()

    def spread(ids, where, value_rows, count):
        size = count * levels
        n = ids.shape[1]
        hot_rows = lax.broadcasted_iota(jnp.int32, (size, n), 0) == ids[where : where + 1, :]
        lanes = lax.broadcasted_iota(jnp.int32, (width, n), 0) == ids[where + 1 : where + 2, :]
        hot = jnp.where(lanes, 1.0, 0.0).astype(jnp.bfloat16)
        out = []
        for value in value_rows:
            rest = jnp.where(hot_rows, value, 0.0)
            total = None
            for _ in range(3):
                part = rest.astype(jnp.bfloat16)
                rest = rest - part.astype(F32)
                term = lax.dot_general(
                    part, hot, (((1,), (1,)), ((), ())), preferred_element_type=F32
                )
                total = term if total is None else total + term
            out.append(total.reshape(count, levels, width))
        return out

    own = spread(cells, 0, [values[i : i + 1, :] for i in range(6)], rows)
    own_s = spread(scells, 0, [svalues[i : i + 1, :] for i in range(2)], rows)
    first[0] = own_s[0]
    second[0, 2 : 2 + rows] = own_s[1]
    for c in range(3):
        first[1 + c] = own[c]
        second[1 + c, 2 : 2 + rows] = own[3 + c]
    for where, at, sign in ((2, 0, north_sign), (4, 2 + rows, south_sign)):
        halo = spread(cells, where, [values[3 + i : 4 + i, :] for i in range(3)], 2)
        second[0, at : at + 2] = spread(scells, where, [svalues[1:2, :]], 2)[0]
        for c in range(3):
            second[1 + c, at : at + 2] = halo[c] * sign if c < 2 else halo[c]


def level_vectors(levels, width, dr, theta_step):
    k = lax.broadcasted_iota(jnp.int32, (levels, width), 0)
    ir = 1.0 / (R_INNER + (k.astype(F32) + 0.5) * dr)
    up = jnp.where(k < levels - 1, 0.5 / dr, 0.0).astype(F32)
    down = jnp.where(k > 0, 0.5 / dr, 0.0).astype(F32)
    return ir, ir * (8.0 / 12.0 / theta_step), ir * (1.0 / 12.0 / theta_step), up, down


def along_theta(ref, k, i, c1, c2):
    return c1 * (ref[k, i + 1] - ref[k, i - 1]) - c2 * (ref[k, i + 2] - ref[k, i - 2])


def along_phi(x):
    return 8.0 * (rolled(x, -1) - rolled(x, 1)) - (rolled(x, -2) - rolled(x, 2))


def along_r(x, up, down):
    return up * rolled(x, -1, 0) - down * rolled(x, 1, 0)


def forces(stress, f, i, vectors, ap, cv):
    ir, c1, c2, up, down = vectors
    k = f * 6
    tt, pp, rr, tp, tr, pr = (stress[k + n, i] for n in range(6))
    f_t = (
        along_theta(stress, k, i, c1, c2)
        + ap * along_phi(tp)
        + along_r(tr, up, down)
        + cv * (tt - pp)
        + 3.0 * (ir * tr)
    )
    f_p = (
        along_theta(stress, k + 3, i, c1, c2)
        + ap * along_phi(pp)
        + along_r(pr, up, down)
        + 2.0 * (cv * tp)
        + 3.0 * (ir * pr)
    )
    f_r = (
        along_theta(stress, k + 4, i, c1, c2)
        + ap * along_phi(pr)
        + along_r(rr, up, down)
        + ir * (2.0 * rr - tt - pp)
        + cv * tr
    )
    return f_t, f_p, f_r


def stress_steps(vel, f, i, vectors, ap, cv, lam, mu2, keep):
    ir, c1, c2, up, down = (v[:, :keep] for v in vectors)
    k = f * 3
    whole = tuple(vel[k + n, i] for n in range(3))
    v_t, v_p, v_r = (x[:, :keep] for x in whole)
    p_t, p_p, p_r = (along_phi(x)[:, :keep] for x in whole)

    def theta(n):
        return c1 * (vel[k + n, i + 1, :, :keep] - vel[k + n, i - 1, :, :keep]) - c2 * (
            vel[k + n, i + 2, :, :keep] - vel[k + n, i - 2, :, :keep]
        )

    ir_r = ir * v_r
    e_tt = theta(0) + ir_r
    e_pp = ap * p_p + cv * v_t + ir_r
    e_rr = along_r(v_r, up, down)
    e_tp = theta(1) - cv * v_p + ap * p_t
    e_tr = along_r(v_t, up, down) - ir * v_t + theta(2)
    e_pr = along_r(v_p, up, down) - ir * v_p + ap * p_r
    bulk = lam * (e_tt + e_pp + e_rr)
    half_mu = 0.5 * mu2
    return (
        bulk + mu2 * e_tt,
        bulk + mu2 * e_pp,
        bulk + mu2 * e_rr,
        half_mu * e_tp,
        half_mu * e_tr,
        half_mu * e_pr,
    )


def look_up(ids, tables, which):
    out = [jnp.zeros(ids.shape, F32) for _ in which]
    for n in range(tables.shape[1]):
        hit = ids == float(n)
        out = [jnp.where(hit, tables[w, n], x) for w, x in zip(which, out)]
    return out


def corners(refs, v):
    _, to_west, to_east = facing()
    ef, eb, wf, wb = (ref[v] for ref in refs)
    return (
        jnp.where(to_east, wf, wb),
        jnp.where(to_west, ef, eb),
        jnp.where(to_east, wb, wf),
        jnp.where(to_west, eb, ef),
    )


def north_south(ref_f, ref_b, k):
    here, _, _ = facing()
    f, b = ref_f[k], ref_b[k]
    return jnp.where(here, f, b), jnp.where(here, b, f)


def velocity_kernel(
    dims, consts, fwd, adj, ids, from_w, from_e, near_f, near_b, d_ef, d_eb, d_wf, d_wb,
    geo, tables, first, stress, vel, pay_f, pay_b, rho,
):
    levels, rows, cols = dims
    dr, theta_step = consts
    width = cols + LANES
    signs = pole_signs()
    here, _, _ = facing()

    for f in range(2):
        source = (fwd, adj)[f]
        for c in range(9):
            for r in range(rows):
                main = strided(source, c * levels * rows + r, levels, rows)
                side = unpack_edges(from_e, from_w, (f * 9 + c) * rows + r)
                if c < 3:
                    ref, k, i = vel, f * 3 + c, r
                else:
                    ref, k, i = stress, f * 6 + c - 3, r + S_ROWS
                ref[k, i, :, :cols] = main
                ref[k, i, :, cols:] = side
    for r in range(rows):
        main = strided(ids, r, levels, rows).astype(F32)
        side = unpack_edges(from_e, from_w, 18 * rows + r)
        rho[r, :, :cols] = look_up(main, tables, (0,))[0]
        rho[r, :, cols:] = look_up(side, tables, (0,))[0]
    per = LANES // EDGE
    for k, (f, c, d) in enumerate(NEAR):
        ne, nw, se, sw = corners((d_ef, d_eb, d_wf, d_wb), k // per)
        north, south = north_south(near_f, near_b, k)
        north_side, south_side = halo_vector(ne, nw, k % per), halo_vector(se, sw, k % per)
        for main, side, i, sign in (
            (north, north_side, S_ROWS - d, signs[0]),
            (south, south_side, S_ROWS + rows - 1 + d, signs[1]),
        ):
            if FIELD_SIGNS[c] < 0:
                main, side = main * sign, side * sign
            stress[f * 6 + c - 3, i, :, :cols] = main
            stress[f * 6 + c - 3, i, :, cols:] = side

    vectors = level_vectors(levels, width, dr, theta_step)

    def step(r, carry):
        i = r + S_ROWS
        ap, cv = vectors[0] * geo[0, i], vectors[0] * geo[1, i]
        scale = rho[r]
        for f in range(2):
            for c, force in enumerate(forces(stress, f, i, vectors, ap, cv)):
                new = vel[f * 3 + c, r] + scale * force
                if f == 1 or c == 2:
                    new = new + first[f * (1 + c), r]
                vel[f * 3 + c, r] = new
        return carry

    lax.fori_loop(0, rows, step, 0)

    tiles = cols // LANES
    packs = Packer(pay_f, 2 * EDGE, len(VEL) * tiles), Packer(pay_b, 2 * EDGE, len(VEL) * tiles)
    for k, (f, c, d) in enumerate(VEL):
        top, bottom = d - 1, rows - d
        for ref, packer, i in (
            (pay_f, packs[0], jnp.where(here, bottom, top)),
            (pay_b, packs[1], jnp.where(here, top, bottom)),
        ):
            x = vel[f * 3 + c, i]
            for t in range(tiles):
                ref[k * tiles + t] = x[:, t * LANES : (t + 1) * LANES]
            packer.add(x[:, cols:], LANES - EDGE)
    for packer in packs:
        packer.flush()


def fill_kernel(
    dims, stress, ids, from_w, from_e, far_f, far_b, d_ef, d_eb, d_wf, d_wb, tables,
    halo, mats,
):
    levels, rows, cols = dims
    signs = pole_signs()
    per = LANES // EDGE

    def sides(k):
        j = k + len(NEAR)
        ne, nw, se, sw = corners((d_ef, d_eb, d_wf, d_wb), j // per)
        north, south = north_south(far_f, far_b, k)
        return (north, halo_vector(ne, nw, j % per)), (south, halo_vector(se, sw, j % per))

    for k, (f, c, d) in enumerate(FAR):
        for (main, side), i, sign in zip(sides(k), (S_ROWS - d, S_ROWS - 1 + d), signs):
            if FIELD_SIGNS[c] < 0:
                main, side = main * sign, side * sign
            halo[f * 6 + c - 3, i, :, :cols] = main
            halo[f * 6 + c - 3, i, :, cols:] = side
    for f, c, d in NEAR:
        k = f * 6 + c - 3
        halo[k, S_ROWS - d] = stress[k, S_ROWS - d]
        halo[k, S_ROWS - 1 + d] = stress[k, S_ROWS + rows - 1 + d]

    def material(i, main, side):
        for x, at in ((main, slice(0, cols)), (side, slice(cols, cols + LANES))):
            for n, value in enumerate(look_up(x, tables, (0, 1, 2))):
                mats[n, i, :, at] = value

    for r in range(rows):
        material(
            r + S_ROWS,
            strided(ids, r, levels, rows).astype(F32),
            unpack_edges(from_e, from_w, 18 * rows + r),
        )
    for d in range(1, S_ROWS + 1):
        for (main, side), i in zip(
            sides(FAR_IDS + d - 1), (S_ROWS - d, S_ROWS + rows - 1 + d)
        ):
            material(i, main, side)


def final_kernel(
    dims, consts, vel_in, stress_in, halo, got_f, got_b, mats, second, geo,
    fwd, adj, density, vel, stress,
):
    levels, rows, cols = dims
    dr, theta_step = consts
    width = cols + LANES
    signs = pole_signs()
    tiles = cols // LANES
    per = LANES // (2 * EDGE)
    for k, (f, c, d) in enumerate(VEL):
        wide = [north_south(got_f, got_b, k * tiles + t) for t in range(tiles)]
        packed = north_south(got_f, got_b, len(VEL) * tiles + k // per)
        for side, i, sign in (
            (0, V_ROWS - d, signs[0]),
            (1, V_ROWS + rows - 1 + d, signs[1]),
        ):
            parts = [w[side] for w in wide]
            parts.append(rolled(packed[side], -EDGE - (k % per) * 2 * EDGE))
            for t, x in enumerate(parts):
                if FIELD_SIGNS[c] < 0:
                    x = x * sign
                vel[f * 3 + c, i, :, t * LANES : (t + 1) * LANES] = x

    for k in range(6):
        for r in range(rows):
            vel[k, V_ROWS + r] = vel_in[k, r]

    vectors = level_vectors(levels, width, dr, theta_step)

    def first_stress(before, shift, i, carry):
        ap, cv = vectors[0] * geo[0, i], vectors[0] * geo[1, i]
        lam, mu2 = mats[1, i], mats[2, i]
        for f in range(2):
            new = stress_steps(
                vel, f, i + V_ROWS - S_ROWS, vectors, ap, cv, lam, mu2, width
            )
            for n in range(6):
                stress[f * 6 + n, i] = before[f * 6 + n, i - shift] + new[n]
        return carry

    inner = S_ROWS + rows
    lax.fori_loop(0, S_ROWS, functools.partial(first_stress, halo, 0), 0)
    lax.fori_loop(S_ROWS, inner, functools.partial(first_stress, stress_in, 0), 0)
    lax.fori_loop(inner, inner + S_ROWS, functools.partial(first_stress, halo, rows), 0)

    def second_velocity(r, carry):
        i = r + S_ROWS - 2
        j = r + V_ROWS - 2
        ap, cv = vectors[0] * geo[0, i], vectors[0] * geo[1, i]
        scale = mats[0, i]
        products = []
        for c in range(3):
            products.append(vel[c, j, :, :cols] * vel[3 + c, j, :, :cols])
        fresh = []
        for f in range(2):
            for c, force in enumerate(forces(stress, f, i, vectors, ap, cv)):
                new = vel[f * 3 + c, j] + scale * force
                if f == 1 or c == 2:
                    new = new + second[f * (1 + c), r]
                vel[f * 3 + c, j] = new
                fresh.append(new[:, :cols])
        for c in range(3):
            products.append(fresh[c] * fresh[3 + c])

        @pl.when(jnp.logical_and(r >= 2, r < rows + 2))
        def _():
            density[pl.ds(r - 2, levels, stride=rows), :] = sum(products[1:], products[0])
            for f in range(2):
                for c in range(3):
                    at = c * levels * rows + r - 2
                    (fwd, adj)[f][pl.ds(at, levels, stride=rows), :] = fresh[f * 3 + c]

        return carry

    lax.fori_loop(0, rows + 4, second_velocity, 0)

    def second_stress(r, carry):
        i = r + S_ROWS
        ap = vectors[0][:, :cols] * geo[0, i]
        cv = vectors[0][:, :cols] * geo[1, i]
        lam, mu2 = mats[1, i, :, :cols], mats[2, i, :, :cols]
        for f in range(2):
            new = stress_steps(vel, f, r + V_ROWS, vectors, ap, cv, lam, mu2, cols)
            for n in range(6):
                at = (3 + n) * levels * rows + r
                (fwd, adj)[f][pl.ds(at, levels, stride=rows), :] = (
                    stress[f * 6 + n, i, :, :cols] + new[n]
                )
        return carry

    lax.fori_loop(0, rows, second_stress, 0)


def row_geometry(first_row, rows, lat_cells, lon_cells):
    ids = first_row + jnp.arange(-S_ROWS, rows + S_ROWS, dtype=jnp.int32)
    beyond = jnp.logical_or(ids < 0, ids >= lat_cells)
    ids = jnp.where(ids < 0, -1 - ids, jnp.where(ids >= lat_cells, 2 * lat_cells - 1 - ids, ids))
    colatitude = (ids.astype(F32) + 0.5) * (math.pi / lat_cells)
    held = jnp.maximum(jnp.sin(colatitude), SIN_FLOOR)
    both = jnp.stack([1.0 / (held * (12.0 * 2.0 * math.pi / lon_cells)), jnp.cos(colatitude) / held])
    return jnp.where(beyond[None, :], -both, both)


def locate(cells, dims, first_row, first_col, lat_cells, lon_cells):
    levels, rows, cols = dims
    plane = lat_cells * lon_cells
    level, row, col = cells // plane, cells % plane // lon_cells, cells % lon_cells
    half = lon_cells // 2
    top, bottom = first_row == 0, first_row + rows == lat_cells

    def lane(c):
        x = (c - first_col + lon_cells) % lon_cells
        before = x - lon_cells + cols + LANES
        return jnp.where(x < cols + EDGE, x, jnp.where(before >= cols + LANES - EDGE, before, -1))

    def code(r, count):
        return jnp.where(jnp.logical_and(r >= 0, r < count), r * levels + level, -1)

    north = 1 - jnp.where(top, row, first_row - 1 - row)
    south = jnp.where(bottom, lat_cells - 1 - row, row - first_row - rows)
    return jnp.stack(
        [
            code(row - first_row, rows),
            lane(col),
            code(north, 2),
            lane(jnp.where(top, col + half, col)),
            code(south, 2),
            lane(jnp.where(bottom, col + half, col)),
        ]
    )


def ring(steps, shift):
    bands, count = lax.axis_size("colat"), lax.axis_size("lon")
    half = count // 2
    pairs = []
    for lon in range(count):
        for band in range(bands):
            down = (lon < half) == (steps > 0)
            to_band, to_lon = band + (1 if down else -1), lon
            if to_band < 0 or to_band >= bands:
                to_band, to_lon = band, (lon + half) % count
            to_lon = (to_lon + shift) % count
            pairs.append((lon * bands + band, to_lon * bands + to_band))
    return pairs


def along_ring(x, steps, shift=0):
    return lax.ppermute(x, ("lon", "colat"), ring(steps, shift))


def along_lon(x, shift):
    count = lax.axis_size("lon")
    return lax.ppermute(x, "lon", [(i, (i + shift) % count) for i in range(count)])


def call(kernel, out_shapes, specs, name, cost=0, **more):
    return pl.pallas_call(
        kernel,
        out_shape=out_shapes,
        in_specs=specs,
        out_specs=jax.tree.map(lambda _: vmem(), out_shapes),
        cost_estimate=pl.CostEstimate(flops=cost, bytes_accessed=cost, transcendentals=0),
        name=name,
        compiler_params=pltpu.CompilerParams(vmem_limit_bytes=16 * 2**20),
        **more,
    )


def on_device(
    forward_state, adjoint_state, layer_ids, density_table, lame_table, shear_table,
    source_cells, source_wavelet, receiver_cells, receiver_residual,
):
    dims = levels, rows, cols = layer_ids.shape
    lat_cells = rows * lax.axis_size("colat")
    lon_cells = cols * lax.axis_size("lon")
    first_row = lax.axis_index("colat") * rows
    first_col = lax.axis_index("lon") * cols
    dt = COURANT * SIN_FLOOR * R_INNER * (2.0 * math.pi / lon_cells) / 1.6
    consts = ((1.0 - R_INNER) / levels, math.pi / lat_cells)
    width = cols + LANES
    tiles = cols // LANES

    def shape(*dims):
        return jax.ShapeDtypeStruct(dims, F32)

    fwd = forward_state.reshape(9 * levels * rows, cols)
    adj = adjoint_state.reshape(9 * levels * rows, cols)
    ids = layer_ids.reshape(levels * rows, cols)

    edges = shape(pieces(19 * rows, EDGE), levels, LANES)
    near = shape(len(NEAR), levels, cols)
    far = shape(len(FAR) + S_ROWS, levels, cols)
    diag = shape(pieces(len(NEAR) + len(FAR) + S_ROWS, EDGE), levels, LANES)
    packed = call(
        functools.partial(pack_kernel, dims),
        [edges, edges, near, near, far, far, diag, diag, diag, diag],
        [vmem()] * 3,
        "pack",
        cost=10**6,
    )(fwd, adj, ids)
    east, west, near_f, near_b, far_f, far_b, d_ef, d_eb, d_wf, d_wb = packed
    near_f, near_b = along_ring(near_f, 1), along_ring(near_b, -1)
    from_w, from_e = along_lon(east, 1), along_lon(west, -1)
    diags = (
        along_ring(d_ef, 1, 1),
        along_ring(d_eb, -1, 1),
        along_ring(d_wf, 1, -1),
        along_ring(d_wb, -1, -1),
    )
    far_f, far_b = along_ring(far_f, 1), along_ring(far_b, -1)

    geo = row_geometry(first_row, rows, lat_cells, lon_cells)
    tables = jnp.stack([dt / density_table, dt * lame_table, (2.0 * dt) * shear_table])
    place = functools.partial(
        locate,
        dims=dims,
        first_row=first_row,
        first_col=first_col,
        lat_cells=lat_cells,
        lon_cells=lon_cells,
    )
    first, second = call(
        functools.partial(inject_kernel, dims),
        [shape(4, rows, levels, width), shape(4, rows + 4, levels, width)],
        [vmem()] * 4,
        "inject",
        cost=10**9,
    )(
        place(receiver_cells),
        receiver_residual.reshape(STEPS * 3, -1),
        place(source_cells),
        source_wavelet,
    )

    payload = shape(len(VEL) * tiles + pieces(len(VEL), 2 * EDGE), levels, LANES)
    stress_shape = shape(12, rows + 2 * S_ROWS, levels, width)
    vel_shape = shape(6, rows, levels, width)
    stress, vel, pay_f, pay_b = call(
        functools.partial(velocity_kernel, dims, consts),
        [stress_shape, vel_shape, payload, payload],
        [vmem()] * 11 + [smem()] * 2 + [vmem()],
        "velocity",
        cost=10**7,
        scratch_shapes=[pltpu.VMEM((rows, levels, width), F32)],
    )(fwd, adj, ids, from_w, from_e, near_f, near_b, *diags, geo, tables, first)
    got_f, got_b = along_ring(pay_f, 1), along_ring(pay_b, -1)

    halo, mats = call(
        functools.partial(fill_kernel, dims),
        [shape(12, 2 * S_ROWS, levels, width), shape(3, rows + 2 * S_ROWS, levels, width)],
        [vmem()] * 10 + [smem()],
        "fill",
        cost=10**8,
    )(stress, ids, from_w, from_e, far_f, far_b, *diags, tables)

    fwd, adj, density = call(
        functools.partial(final_kernel, dims, consts),
        [shape(*fwd.shape), shape(*adj.shape), shape(*ids.shape)],
        [vmem()] * 7 + [smem()],
        "final",
        cost=10**8,
        scratch_shapes=[
            pltpu.VMEM((6, rows + 2 * V_ROWS, levels, width), F32),
            pltpu.VMEM(stress_shape.shape, F32),
        ],
    )(vel, stress, halo, got_f, got_b, mats, second, geo)
    return (
        fwd.reshape(forward_state.shape),
        adj.reshape(adjoint_state.shape),
        density.reshape(layer_ids.shape),
    )


def solution(mesh):
    return jax.shard_map(
        on_device,
        mesh=mesh,
        in_specs=(
            P(None, None, "colat", "lon"),
            P(None, None, "colat", "lon"),
            P(None, "colat", "lon"),
        )
        + (P(),) * 7,
        out_specs=(
            P(None, None, "colat", "lon"),
            P(None, None, "colat", "lon"),
            P(None, "colat", "lon"),
        ),
        check_vma=False,
    )
```

```python
import functools
import math

import jax
import jax.numpy as jnp
from jax import lax
from jax.experimental import pallas as pl
from jax.experimental.pallas import tpu as pltpu
from jax.sharding import PartitionSpec as P

R_INNER = 0.55
COURANT = 0.3
SIN_FLOOR = 0.25
FIELD_SIGNS = (-1, -1, 1, 1, 1, 1, 1, -1, -1)
CROSS = (3, 6, 7)
OTHER = (4, 5, 8)
EDGE = 8
LANES = 128
V_ROWS = 6
S_ROWS = 4
F32 = jnp.float32


NEAR = tuple((f, c, d) for f in range(2) for c in CROSS for d in (1, 2))
FAR = tuple((f, c, d) for f in range(2) for c in OTHER for d in (1, 2)) + tuple(
    (f, c, d) for f in range(2) for c in CROSS for d in (3, 4)
)
FAR_IDS = len(FAR)
VEL = tuple((f, c, d) for f in range(2) for c in range(3) for d in range(1, V_ROWS + 1))


def vmem():
    return pl.BlockSpec(memory_space=pltpu.VMEM)


def smem():
    return pl.BlockSpec(memory_space=pltpu.SMEM)


def lane_iota(shape):
    return lax.broadcasted_iota(jnp.int32, shape, 1)


def rolled(x, shift, axis=1):
    size = x.shape[axis]
    shift = shift % size
    return x if shift == 0 else pltpu.roll(x, shift, axis)


class Packer:
    def __init__(self, ref, width, base=0):
        self.ref, self.width, self.base = ref, width, base
        self.per = LANES // width
        self.count, self.value = 0, None

    def add(self, x, start):
        slot = self.count % self.per
        moved = rolled(x, slot * self.width - start)
        if slot == 0:
            self.value = moved
        else:
            self.value = jnp.where(lane_iota(x.shape) >= slot * self.width, moved, self.value)
        self.count += 1
        if self.count % self.per == 0:
            self.flush()

    def flush(self):
        if self.value is not None:
            self.ref[self.base + (self.count - 1) // self.per] = self.value
            self.value = None


def pieces(count, width):
    per = LANES // width
    return -(-count // per)


def halo_vector(east, west, slot):
    after = rolled(east, -slot * EDGE)
    before = rolled(west, LANES - EDGE - slot * EDGE)
    return jnp.where(lane_iota(after.shape) < LANES // 2, after, before)


def even_band():
    return lax.rem(lax.axis_index("colat"), 2) == 0


def even_tile():
    return lax.rem(lax.axis_index("lon"), 2) == 0


def pole_signs():
    band, last = lax.axis_index("colat"), lax.axis_size("colat") - 1
    north = jnp.where(band == 0, -1.0, 1.0).astype(F32)
    south = jnp.where(band == last, -1.0, 1.0).astype(F32)
    return north, south


def strided(ref, first, levels, rows):
    return ref[pl.ds(first, levels, stride=rows), :]


def pack_kernel(dims, state, edge_a, edge_b, near_a, near_b, far_a, far_b):
    levels, rows, cols = dims
    even = even_band()

    def row(f, c, r):
        return strided(state, (f * 9 + c) * levels * rows + r, levels, rows)

    def id_row(r):
        return strided(state, 18 * levels * rows + r, levels, rows)

    def put(ref_a, ref_b, k, get, d):
        top, bottom = get(d - 1), get(rows - d)
        ref_a[k], ref_b[k] = jnp.where(even, bottom, top), jnp.where(even, top, bottom)

    for k, (f, c, d) in enumerate(NEAR):
        put(near_a, near_b, k, functools.partial(row, f, c), d)
    for k, (f, c, d) in enumerate(FAR):
        put(far_a, far_b, k, functools.partial(row, f, c), d)
    for d in range(1, S_ROWS + 1):
        put(far_a, far_b, FAR_IDS + d - 1, id_row, d)

    east, west = Packer(edge_a, EDGE), Packer(edge_b, EDGE)

    def both(x):
        east.add(x[:, cols - LANES :], LANES - EDGE)
        west.add(x[:, :LANES], 0)

    for f in range(2):
        for c in range(9):
            for r in range(rows):
                both(row(f, c, r))
    for r in range(rows):
        both(id_row(r))
    east.flush()
    west.flush()

    @pl.when(jnp.logical_not(even_tile()))
    def _():
        for v in range(edge_a.shape[0]):
            edge_a[v], edge_b[v] = edge_b[v], edge_a[v]


def divided(x, by):
    q = jnp.floor(x.astype(F32) * (1.0 / by)).astype(jnp.int32)
    r = x - q * by
    q = q + jnp.where(r >= by, 1, 0) - jnp.where(r < 0, 1, 0)
    return q, x - q * by


def inject(dims, extents, step, given, out, halo):
    levels, rows, cols = dims
    lat_cells, lon_cells = extents
    width = cols + LANES
    north_sign, south_sign = pole_signs()
    first_row, first_col = lax.axis_index("colat") * rows, lax.axis_index("lon") * cols
    at_top, at_bottom = first_row == 0, first_row + rows == lat_cells
    half = lon_cells // 2

    def located(ids):
        level, rest = divided(ids, lat_cells * lon_cells)
        row, col = divided(rest, lon_cells)

        def lane(c):
            x = c - first_col
            x = jnp.where(x < 0, x + lon_cells, x)
            x = jnp.where(x >= lon_cells, x - lon_cells, x)
            tail = x - lon_cells + cols + LANES
            tail = jnp.where(tail >= cols + LANES - EDGE, tail, -1)
            return jnp.where(x < cols + EDGE, x, tail)

        def code(r, count):
            inside = jnp.logical_and(r >= 0, r < count)
            return jnp.where(inside, r * levels + level, -1)

        north = 1 - jnp.where(at_top, row, first_row - 1 - row)
        south = jnp.where(at_bottom, lat_cells - 1 - row, row - first_row - rows)
        return (
            (code(row - first_row, rows), lane(col)),
            (code(north, 2), lane(jnp.where(at_top, col + half, col))),
            (code(south, 2), lane(jnp.where(at_bottom, col + half, col))),
        )

    def spread(place, value_rows, count):
        code, lane = place
        n = code.shape[1]
        hot_rows = lax.broadcasted_iota(jnp.int32, (count * levels, n), 0) == code
        hot = lax.broadcasted_iota(jnp.int32, (width, n), 0) == lane
        hot = jnp.where(hot, 1.0, 0.0).astype(jnp.bfloat16)
        out = []
        for value in value_rows:
            rest = jnp.where(hot_rows, value, 0.0)
            total = None
            for _ in range(3):
                part = rest.astype(jnp.bfloat16)
                rest = rest - part.astype(F32)
                term = lax.dot_general(
                    part, hot, (((1,), (1,)), ((), ())), preferred_element_type=F32
                )
                total = term if total is None else total + term
            out.append(total.reshape(count, levels, width))
        return out

    places = located(given[0:1, :].astype(jnp.int32))
    splaces = located(given[7:8, :LANES].astype(jnp.int32))
    values = [given[1 + 3 * step + c : 2 + 3 * step + c, :] for c in range(3)]
    svalues = [given[8 + step : 9 + step, :LANES]]
    regions = ((0, halo, rows, 1.0), (1, 0, halo, north_sign), (2, halo + rows, halo, south_sign))
    for where, at, count, sign in regions:
        if count:
            out[0, at : at + count] = spread(splaces[where], svalues, count)[0]
            for c, got in enumerate(spread(places[where], values, count)):
                signed = where and FIELD_SIGNS[c] < 0
                out[1 + c, at : at + count] = got * sign if signed else got


def first_inject_kernel(dims, extents, given, out, ap, cv):
    levels, rows, _ = dims
    lat_cells, lon_cells = extents
    first_row = lax.axis_index("colat") * rows
    inject(dims, extents, 0, given, out, 0)
    deep = rows + 2 * S_ROWS
    g = lax.broadcasted_iota(jnp.int32, (deep, LANES), 0) + (first_row - S_ROWS)
    sign = jnp.where(jnp.logical_or(g < 0, g >= lat_cells), -1.0, 1.0)
    g = jnp.where(g < 0, -1 - g, jnp.where(g >= lat_cells, 2 * lat_cells - 1 - g, g))
    angle = (g.astype(F32) + 0.5) * (math.pi / lat_cells)
    held = jnp.maximum(jnp.sin(angle), SIN_FLOOR)
    across = sign / (held * (24.0 * math.pi / lon_cells))
    cot = sign * jnp.cos(angle) / held
    ir = level_vectors(levels, LANES, (1.0 - R_INNER) / levels, math.pi / lat_cells)[0]
    for i in range(deep):
        ap[i] = ir * across[i : i + 1, :]
        cv[i] = ir * cot[i : i + 1, :]


def second_inject_kernel(dims, extents, given, out):
    inject(dims, extents, 1, given, out, 2)


def level_vectors(levels, width, dr, theta_step):
    k = lax.broadcasted_iota(jnp.int32, (levels, width), 0)
    ir = 1.0 / (R_INNER + (k.astype(F32) + 0.5) * dr)
    up = jnp.where(k < levels - 1, 0.5 / dr, 0.0).astype(F32)
    down = jnp.where(k > 0, 0.5 / dr, 0.0).astype(F32)
    return ir, ir * (8.0 / 12.0 / theta_step), ir * (1.0 / 12.0 / theta_step), up, down


def along_theta(ref, k, i, c1, c2):
    return c1 * (ref[k, i + 1] - ref[k, i - 1]) - c2 * (ref[k, i + 2] - ref[k, i - 2])


def along_phi(x):
    return 8.0 * (rolled(x, -1) - rolled(x, 1)) - (rolled(x, -2) - rolled(x, 2))


def along_r(x, up, down):
    return up * rolled(x, -1, 0) - down * rolled(x, 1, 0)


def forces(stress, f, i, vectors, ap, cv):
    ir, c1, c2, up, down = vectors
    k = f * 6
    tt, pp, rr, tp, tr, pr = (stress[k + n, i] for n in range(6))
    f_t = (
        along_theta(stress, k, i, c1, c2)
        + ap * along_phi(tp)
        + along_r(tr, up, down)
        + cv * (tt - pp)
        + 3.0 * (ir * tr)
    )
    f_p = (
        along_theta(stress, k + 3, i, c1, c2)
        + ap * along_phi(pp)
        + along_r(pr, up, down)
        + 2.0 * (cv * tp)
        + 3.0 * (ir * pr)
    )
    f_r = (
        along_theta(stress, k + 4, i, c1, c2)
        + ap * along_phi(pr)
        + along_r(rr, up, down)
        + ir * (2.0 * rr - tt - pp)
        + cv * tr
    )
    return f_t, f_p, f_r


def stress_steps(vel, f, i, vectors, ap, cv, lam, mu2, keep):
    ir, c1, c2, up, down = (v[:, :keep] for v in vectors)
    k = f * 3
    whole = tuple(vel[k + n, i] for n in range(3))
    v_t, v_p, v_r = (x[:, :keep] for x in whole)
    p_t, p_p, p_r = (along_phi(x)[:, :keep] for x in whole)

    def theta(n):
        return c1 * (vel[k + n, i + 1, :, :keep] - vel[k + n, i - 1, :, :keep]) - c2 * (
            vel[k + n, i + 2, :, :keep] - vel[k + n, i - 2, :, :keep]
        )

    ir_r = ir * v_r
    e_tt = theta(0) + ir_r
    e_pp = ap * p_p + cv * v_t + ir_r
    e_rr = along_r(v_r, up, down)
    e_tp = theta(1) - cv * v_p + ap * p_t
    e_tr = along_r(v_t, up, down) - ir * v_t + theta(2)
    e_pr = along_r(v_p, up, down) - ir * v_p + ap * p_r
    bulk = lam * (e_tt + e_pp + e_rr)
    half_mu = 0.5 * mu2
    return (
        bulk + mu2 * e_tt,
        bulk + mu2 * e_pp,
        bulk + mu2 * e_rr,
        half_mu * e_tp,
        half_mu * e_tr,
        half_mu * e_pr,
    )


def look_up(ids, tables):
    out = [jnp.full(ids.shape, table[0], F32) for table in tables]
    for n in range(1, tables[0].shape[0]):
        hit = ids == float(n)
        out = [jnp.where(hit, table[n], x) for table, x in zip(tables, out)]
    return out


def materials(ids, dt, tables):
    rho, lam, mu = look_up(ids, tables)
    return dt / rho, dt * lam, (2.0 * dt) * mu


def widened(x, width):
    return jnp.concatenate([x] * (width // LANES), axis=1)


def north_south(ref_a, ref_b, k):
    even = even_band()
    a, b = ref_a[k], ref_b[k]
    return jnp.where(even, b, a), jnp.where(even, a, b)


def velocity_kernel(
    dims, consts, state, edge_a, edge_b, near_a, near_b, ap, cv, first, density,
    stress, vel, pay_a, pay_b, rho, id_side,
):
    levels, rows, cols = dims
    dr, theta_step, dt = consts
    width = cols + LANES
    signs = pole_signs()
    even = even_band()
    per = LANES // EDGE
    east_first = even_tile()

    def side_of(j):
        a, b = edge_a[j // per], edge_b[j // per]
        return halo_vector(jnp.where(east_first, a, b), jnp.where(east_first, b, a), j % per)

    for f in range(2):
        for c in range(9):
            for r in range(rows):
                main = strided(state, (f * 9 + c) * levels * rows + r, levels, rows)
                side = side_of((f * 9 + c) * rows + r)
                if c < 3:
                    ref, k, i = vel, f * 3 + c, r
                else:
                    ref, k, i = stress, f * 6 + c - 3, r + S_ROWS
                ref[k, i, :, :cols] = main
                ref[k, i, :, cols:] = side
    for r in range(rows):
        main = strided(state, 18 * levels * rows + r, levels, rows)
        side = side_of(18 * rows + r)
        id_side[r] = side
        rho[r, :, :cols] = dt / look_up(main, (density,))[0]
        rho[r, :, cols:] = dt / look_up(side, (density,))[0]
    for k, (f, c, d) in enumerate(NEAR):
        for main, i, sign in zip(
            north_south(near_a, near_b, k), (S_ROWS - d, S_ROWS + rows - 1 + d), signs
        ):
            if FIELD_SIGNS[c] < 0:
                main = main * sign
            stress[f * 6 + c - 3, i, :, :cols] = main
            stress[f * 6 + c - 3, i, :, cols:] = jnp.zeros((levels, LANES), F32)

    vectors = level_vectors(levels, width, dr, theta_step)

    def step(r, carry):
        i = r + S_ROWS
        scale = rho[r]
        row_ap, row_cv = widened(ap[i], width), widened(cv[i], width)
        for f in range(2):
            for c, force in enumerate(forces(stress, f, i, vectors, row_ap, row_cv)):
                new = vel[f * 3 + c, r] + scale * force
                if f == 1 or c == 2:
                    new = new + first[f * (1 + c), r]
                vel[f * 3 + c, r] = new
        return carry

    lax.fori_loop(0, rows, step, 0, unroll=2)

    tiles = cols // LANES
    for ref, bottom_side in ((pay_a, even), (pay_b, jnp.logical_not(even))):
        packer = Packer(ref, 2 * EDGE, len(VEL) * tiles)

        def facing(d):
            return jnp.where(bottom_side, rows - d, d - 1)

        for k, (f, c, d) in enumerate(VEL):
            x = vel[f * 3 + c, facing(d)]
            for t in range(tiles):
                ref[k * tiles + t] = x[:, t * LANES : (t + 1) * LANES]
            packer.add(x[:, cols:], LANES - EDGE)
        for f, c, d in NEAR + FAR:
            packer.add(stress[f * 6 + c - 3, facing(d) + S_ROWS, :, cols:], LANES - EDGE)
        for d in range(1, S_ROWS + 1):
            packer.add(id_side[facing(d)], LANES - EDGE)
        packer.flush()


def fill_kernel(
    dims, dt, stress, state, id_edge_a, id_edge_b, far_a, far_b, density, lame, shear,
    halo, mats,
):
    levels, rows, cols = dims
    signs = pole_signs()
    tables = density, lame, shear
    per = LANES // EDGE
    east_first = even_tile()

    for k, (f, c, d) in enumerate(FAR):
        for main, i, sign in zip(
            north_south(far_a, far_b, k), (S_ROWS - d, S_ROWS - 1 + d), signs
        ):
            halo[f * 6 + c - 3, i] = main * sign if FIELD_SIGNS[c] < 0 else main
    for f, c, d in NEAR:
        k = f * 6 + c - 3
        halo[k, S_ROWS - d] = stress[k, S_ROWS - d, :, :cols]
        halo[k, S_ROWS - 1 + d] = stress[k, S_ROWS + rows - 1 + d, :, :cols]

    def material(i, x, at):
        for n, value in enumerate(materials(x, dt, tables)):
            mats[n, i, :, at] = value

    main, side = slice(0, cols), slice(cols, cols + LANES)
    for r in range(rows):
        material(r + S_ROWS, strided(state, 18 * levels * rows + r, levels, rows), main)
        j = 18 * rows + r
        a, b = id_edge_a[j // per], id_edge_b[j // per]
        x = halo_vector(jnp.where(east_first, a, b), jnp.where(east_first, b, a), j % per)
        material(r + S_ROWS, x, side)
    for d in range(1, S_ROWS + 1):
        north, south = north_south(far_a, far_b, FAR_IDS + d - 1)
        material(S_ROWS - d, north, main)
        material(S_ROWS + rows - 1 + d, south, main)


def final_kernel(
    dims, consts, vel_in, stress_in, halo, got_a, got_b, mats_in, second, ap, cv,
    density_t, lame_t, shear_t, fwd, adj, density, vel, stress, mats,
):
    levels, rows, cols = dims
    dr, theta_step, dt = consts
    width = cols + LANES
    signs = pole_signs()
    tiles = cols // LANES
    per = LANES // (2 * EDGE)
    even = even_band()
    side_at = slice(cols, width)

    def sides(j):
        v = len(VEL) * tiles + j // per
        return (
            rolled(x, -EDGE - (j % per) * 2 * EDGE) for x in north_south(got_a, got_b, v)
        )

    for k, (f, c, d) in enumerate(VEL):
        flip = FIELD_SIGNS[c] < 0
        for t in range(tiles):
            at = slice(t * LANES, (t + 1) * LANES)
            north, south = north_south(got_a, got_b, k * tiles + t)
            vel[f * 3 + c, V_ROWS - d, :, at] = north * signs[0] if flip else north
            vel[f * 3 + c, V_ROWS + rows - 1 + d, :, at] = south * signs[1] if flip else south
        for x, i, sign in zip(sides(k), (V_ROWS - d, V_ROWS + rows - 1 + d), signs):
            vel[f * 3 + c, i, :, side_at] = x * sign if flip else x
    for k, (f, c, d) in enumerate(NEAR + FAR):
        n = f * 6 + c - 3
        for x, i, i_main, sign in zip(
            sides(len(VEL) + k),
            (S_ROWS - d, S_ROWS + rows - 1 + d),
            (S_ROWS - d, S_ROWS - 1 + d),
            signs,
        ):
            stress[n, i, :, side_at] = x * sign if FIELD_SIGNS[c] < 0 else x
            stress[n, i, :, :cols] = halo[n, i_main]
    for d in range(1, S_ROWS + 1):
        for x, i in zip(
            sides(len(VEL + NEAR + FAR) + d - 1), (S_ROWS - d, S_ROWS + rows - 1 + d)
        ):
            for n, value in enumerate(materials(x, dt, (density_t, lame_t, shear_t))):
                mats[n, i, :, side_at] = value
                mats[n, i, :, :cols] = mats_in[n, i, :, :cols]
    for n in range(3):
        for r in range(rows):
            mats[n, S_ROWS + r] = mats_in[n, S_ROWS + r]
    for k in range(6):
        for r in range(rows):
            vel[k, V_ROWS + r] = vel_in[k, r]

    vectors = level_vectors(levels, width, dr, theta_step)
    c1, c2 = vectors[1][:, :LANES], vectors[2][:, :LANES]

    def add_side(k, r, value):
        scale = mats[0, S_ROWS + r, :, side_at]
        vel[k, V_ROWS + r, :, side_at] = vel[k, V_ROWS + r, :, side_at] + scale * value

    for f in range(2):
        for c in range(3):
            k, n = f * 3 + c, f * 6 + CROSS[c] - 3
            n1, n2 = (stress[n, S_ROWS - d, :, side_at] for d in (1, 2))
            s1, s2 = (stress[n, S_ROWS + rows - 1 + d, :, side_at] for d in (1, 2))
            o1, o2 = (stress_in[n, S_ROWS + d, :, side_at] for d in (0, 1))
            u1, u2 = (stress_in[n, S_ROWS + rows - d, :, side_at] for d in (1, 2))
            add_side(k, 0, c2 * n2 - c1 * n1)
            add_side(k, 1, c2 * n1)
            add_side(k, rows - 1, c1 * s1 - c2 * s2)
            add_side(k, rows - 2, -(c2 * s1))
            add_side(k, -1, c1 * o1 - c2 * o2)
            add_side(k, -2, -(c2 * o1))
            add_side(k, rows, c2 * u2 - c1 * u1)
            add_side(k, rows + 1, c2 * u1)

    def first_stress(before, i, carry):
        row_ap, row_cv = widened(ap[i], width), widened(cv[i], width)
        lam, mu2 = mats[1, i], mats[2, i]
        for f in range(2):
            new = stress_steps(
                vel, f, i + V_ROWS - S_ROWS, vectors, row_ap, row_cv, lam, mu2, width
            )
            for n in range(6):
                stress[f * 6 + n, i] = before[f * 6 + n, i] + new[n]
        return carry

    inner = S_ROWS + rows
    lax.fori_loop(0, S_ROWS, functools.partial(first_stress, stress), 0, unroll=4)
    lax.fori_loop(S_ROWS, inner, functools.partial(first_stress, stress_in), 0, unroll=4)
    lax.fori_loop(inner, inner + S_ROWS, functools.partial(first_stress, stress), 0, unroll=4)

    def second_velocity(own, r, carry):
        i = r + S_ROWS - 2
        j = r + V_ROWS - 2
        row_ap, row_cv = widened(ap[i], width), widened(cv[i], width)
        scale = mats[0, i]
        fresh, products = [], []
        if own:
            for c in range(3):
                products.append(vel[c, j, :, :cols] * vel[3 + c, j, :, :cols])
        for f in range(2):
            for c, force in enumerate(forces(stress, f, i, vectors, row_ap, row_cv)):
                new = vel[f * 3 + c, j] + scale * force
                if f == 1 or c == 2:
                    new = new + second[f * (1 + c), r]
                vel[f * 3 + c, j] = new
                fresh.append(new[:, :cols])
        if own:
            for c in range(3):
                products.append(fresh[c] * fresh[3 + c])
            density[pl.ds(r - 2, levels, stride=rows), :] = sum(products[1:], products[0])
            for f in range(2):
                for c in range(3):
                    at = c * levels * rows + r - 2
                    (fwd, adj)[f][pl.ds(at, levels, stride=rows), :] = fresh[f * 3 + c]
        return carry

    lax.fori_loop(0, 2, functools.partial(second_velocity, False), 0, unroll=2)
    lax.fori_loop(2, rows + 2, functools.partial(second_velocity, True), 0, unroll=4)
    lax.fori_loop(rows + 2, rows + 4, functools.partial(second_velocity, False), 0, unroll=2)

    def second_stress(r, carry):
        i = r + S_ROWS
        row_ap, row_cv = widened(ap[i], cols), widened(cv[i], cols)
        lam, mu2 = mats[1, i, :, :cols], mats[2, i, :, :cols]
        for f in range(2):
            new = stress_steps(vel, f, r + V_ROWS, vectors, row_ap, row_cv, lam, mu2, cols)
            for n in range(6):
                at = (3 + n) * levels * rows + r
                (fwd, adj)[f][pl.ds(at, levels, stride=rows), :] = (
                    stress[f * 6 + n, i, :, :cols] + new[n]
                )
        return carry

    lax.fori_loop(0, rows, second_stress, 0, unroll=4)


def swap_tiles(x, first):
    count = lax.axis_size("lon")
    to = {i: (i + (1 if (i % 2 == 0) == first else -1)) % count for i in range(count)}
    return lax.ppermute(x, "lon", list(to.items()))


def swap_bands(x, first):
    bands, count = lax.axis_size("colat"), lax.axis_size("lon")
    pairs = []
    for lon in range(count):
        for band in range(bands):
            to_band, to_lon = band + (1 if (band % 2 == 0) == first else -1), lon
            if to_band < 0 or to_band >= bands:
                to_band, to_lon = band, (lon + count // 2) % count
            pairs.append((lon * bands + band, to_lon * bands + to_band))
    return lax.ppermute(x, ("lon", "colat"), pairs)


def call(kernel, out_shapes, specs, cost=0, limit=16 * 2**20, **more):
    return pl.pallas_call(
        kernel,
        out_shape=out_shapes,
        in_specs=specs,
        out_specs=jax.tree.map(lambda _: vmem(), out_shapes),
        cost_estimate=pl.CostEstimate(flops=cost, bytes_accessed=cost, transcendentals=0),
        compiler_params=pltpu.CompilerParams(vmem_limit_bytes=limit),
        **more,
    )


def on_device(
    forward_state, adjoint_state, layer_ids, density_table, lame_table, shear_table,
    source_cells, source_wavelet, receiver_cells, receiver_residual,
):
    dims = levels, rows, cols = layer_ids.shape
    lat_cells = rows * lax.axis_size("colat")
    lon_cells = cols * lax.axis_size("lon")
    dt = COURANT * SIN_FLOOR * R_INNER * (2.0 * math.pi / lon_cells) / 1.6
    consts = ((1.0 - R_INNER) / levels, math.pi / lat_cells, dt)
    width = cols + LANES
    tiles = cols // LANES

    def shape(*dims):
        return jax.ShapeDtypeStruct(dims, F32)

    parts = forward_state, adjoint_state, layer_ids.astype(F32)
    state = jnp.concatenate([x.reshape(-1, rows, cols) for x in parts]).reshape(-1, cols)

    edges = shape(pieces(19 * rows, EDGE), levels, LANES)
    near = shape(len(NEAR), levels, cols)
    far = shape(len(FAR) + S_ROWS, levels, cols)
    edge_a, edge_b, near_a, near_b, far_a, far_b = call(
        functools.partial(pack_kernel, dims),
        [edges, edges, near, near, far, far],
        [vmem()],
        cost=10**6,
    )(state)
    near_b, near_a = swap_bands(near_b, False), swap_bands(near_a, True)
    edge_b, edge_a = swap_tiles(edge_b, False), swap_tiles(edge_a, True)
    far_b = swap_bands(far_b, False)
    far_a = swap_bands(far_a, True)

    deep = shape(rows + 2 * S_ROWS, levels, LANES)
    count = max(LANES, receiver_cells.shape[0])

    def lines(x):
        x = x.astype(F32).reshape(-1, x.shape[-1])
        return jnp.pad(x, ((0, 0), (0, count - x.shape[1])))

    given = jnp.concatenate(
        [lines(x) for x in (receiver_cells, receiver_residual, source_cells, source_wavelet)]
    )
    extents = lat_cells, lon_cells
    first, ap, cv = call(
        functools.partial(first_inject_kernel, dims, extents),
        [shape(4, rows, levels, width), deep, deep],
        [vmem()],
        cost=10**8,
    )(given)

    extra = len(VEL + NEAR + FAR) + S_ROWS
    payload = shape(len(VEL) * tiles + pieces(extra, 2 * EDGE), levels, LANES)
    stress_shape = shape(12, rows + 2 * S_ROWS, levels, width)
    mats_shape = shape(3, rows + 2 * S_ROWS, levels, width)
    stress, vel, pay_a, pay_b = call(
        functools.partial(velocity_kernel, dims, consts),
        [stress_shape, shape(6, rows, levels, width), payload, payload],
        [vmem()] * 8 + [smem()],
        cost=10**7,
        scratch_shapes=[
            pltpu.VMEM((rows, levels, width), F32),
            pltpu.VMEM((rows, levels, LANES), F32),
        ],
    )(state, edge_a, edge_b, near_a, near_b, ap, cv, first, density_table)
    got_b, got_a = swap_bands(pay_b, False), swap_bands(pay_a, True)

    second = call(
        functools.partial(second_inject_kernel, dims, extents),
        shape(4, rows + 4, levels, width),
        [vmem()],
        cost=10**8,
    )(given)
    halo, mats = call(
        functools.partial(fill_kernel, dims, dt),
        [shape(12, 2 * S_ROWS, levels, cols), mats_shape],
        [vmem()] * 6 + [smem()] * 3,
        cost=10**8,
    )(stress, state, edge_a, edge_b, far_a, far_b, density_table, lame_table, shear_table)

    fwd, adj, density = call(
        functools.partial(final_kernel, dims, consts),
        [shape(9 * levels * rows, cols)] * 2 + [shape(levels * rows, cols)],
        [vmem()] * 9 + [smem()] * 3,
        cost=10**8,
        scratch_shapes=[
            pltpu.VMEM((6, rows + 2 * V_ROWS, levels, width), F32),
            pltpu.VMEM(stress_shape.shape, F32),
            pltpu.VMEM(mats_shape.shape, F32),
        ],
    )(
        vel, stress, halo, got_a, got_b, mats, second, ap, cv,
        density_table, lame_table, shear_table,
    )
    return (
        fwd.reshape(forward_state.shape),
        adj.reshape(adjoint_state.shape),
        density.reshape(layer_ids.shape),
    )


def solution(mesh):
    return jax.shard_map(
        on_device,
        mesh=mesh,
        in_specs=(
            P(None, None, "colat", "lon"),
            P(None, None, "colat", "lon"),
            P(None, "colat", "lon"),
        )
        + (P(),) * 7,
        out_specs=(
            P(None, None, "colat", "lon"),
            P(None, None, "colat", "lon"),
            P(None, "colat", "lon"),
        ),
        check_vma=False,
    )
```

```python
import functools
import math

import jax
import jax.numpy as jnp
from jax import lax
from jax.experimental import pallas as pl
from jax.experimental.pallas import tpu as pltpu
from jax.sharding import PartitionSpec as P

R_INNER = 0.55
COURANT = 0.3
SIN_FLOOR = 0.25
FIELD_SIGNS = (-1, -1, 1, 1, 1, 1, 1, -1, -1)
CROSS = (3, 6, 7)
OTHER = (4, 5, 8)
EDGE = 8
LANES = 128
V_ROWS = 6
S_ROWS = 4
INNER = 4
F32 = jnp.float32


NEAR = tuple((f, c, d) for f in range(2) for c in CROSS for d in (1, 2))
FAR = tuple((f, c, d) for f in range(2) for c in OTHER for d in (1, 2)) + tuple(
    (f, c, d) for f in range(2) for c in CROSS for d in (3, 4)
)
FAR_IDS = len(FAR)
VEL = tuple((f, c, d) for f in range(2) for c in range(3) for d in range(1, V_ROWS + 1))


def vmem():
    return pl.BlockSpec(memory_space=pltpu.VMEM)


def smem():
    return pl.BlockSpec(memory_space=pltpu.SMEM)


def lane_iota(shape):
    return lax.broadcasted_iota(jnp.int32, shape, 1)


def rolled(x, shift, axis=1):
    size = x.shape[axis]
    shift = shift % size
    return x if shift == 0 else pltpu.roll(x, shift, axis)


def side_plan():
    wide = [("v", f, c, 1) for f in range(2) for c in range(3)]
    wide += [("s",) + entry for entry in NEAR] + [("i", 0, 0, 1)]
    slim = [("v", f, c, d) for f, c, d in VEL if 1 < d < V_ROWS]
    slim += [("s",) + entry for entry in FAR if entry[2] < S_ROWS] + [("i", 0, 0, 2), ("i", 0, 0, 3)]
    plan, lane = {}, 0
    for width, entries in ((2 * EDGE, wide), (EDGE, slim)):
        for entry in entries:
            plan[entry] = (lane // LANES, lane % LANES, width)
            lane += width
    return plan, -(-lane // LANES)


def pieces(count, width):
    per = LANES // width
    return -(-count // per)


def paired_edges(edge_a, edge_b, v):
    a, b = edge_a[v], edge_b[v]
    even = even_tile()
    after, before = jnp.where(even, a, b), jnp.where(even, b, a)
    odd_lane = lax.rem(lane_iota(a.shape) // EDGE, 2) == 1
    return jnp.where(odd_lane, before, after), jnp.where(odd_lane, after, before)


def side_vector(paired, slot):
    return rolled(paired[slot % 2], -slot * EDGE)


def even_band():
    return lax.rem(lax.axis_index("colat"), 2) == 0


def even_tile():
    return lax.rem(lax.axis_index("lon"), 2) == 0


def pole_signs():
    band, last = lax.axis_index("colat"), lax.axis_size("colat") - 1
    north = jnp.where(band == 0, -1.0, 1.0).astype(F32)
    south = jnp.where(band == last, -1.0, 1.0).astype(F32)
    return north, south


def strided(ref, first, levels, rows):
    return ref[pl.ds(first, levels, stride=rows), :]


def pack_kernel(dims, state, ids, edge_a, edge_b, near_a, near_b, far_a, far_b):
    levels, rows, cols = dims
    even = even_band()

    def row(f, c, r):
        return strided(state, (f * 9 + c) * levels * rows + r, levels, rows)

    def id_row(r):
        return strided(ids, r, levels, rows).astype(F32)

    def put(ref_a, ref_b, k, get, d):
        top, bottom = get(d - 1), get(rows - d)
        ref_a[k], ref_b[k] = jnp.where(even, bottom, top), jnp.where(even, top, bottom)

    for k, (f, c, d) in enumerate(NEAR):
        put(near_a, near_b, k, functools.partial(row, f, c), d)
    for k, (f, c, d) in enumerate(FAR):
        put(far_a, far_b, k, functools.partial(row, f, c), d)
    for d in range(1, S_ROWS + 1):
        put(far_a, far_b, FAR_IDS + d - 1, id_row, d)

    per = LANES // EDGE
    edges = [functools.partial(row, f, c, r) for f in range(2) for c in range(9) for r in range(rows)]
    edges += [functools.partial(id_row, r) for r in range(rows)]
    lane = lane_iota((levels, LANES))
    swapped = jnp.logical_not(even_tile())
    for v in range(edge_a.shape[0]):
        east = west = None
        for slot, get in reversed(list(enumerate(edges[v * per : (v + 1) * per]))):
            x = get()
            last = rolled(x[:, cols - LANES :], slot * EDGE)
            first = last if cols == LANES else rolled(x[:, :LANES], slot * EDGE)
            if east is None:
                east, west = last, first
            else:
                west = jnp.where(lane < (slot + 1) * EDGE, first, west)
                if slot:
                    east = jnp.where(lane < slot * EDGE, last, east)
                else:
                    east = jnp.where(lane < LANES - EDGE, east, last)
        edge_a[v] = jnp.where(swapped, west, east)
        edge_b[v] = jnp.where(swapped, east, west)


def divided(x, by):
    q = jnp.floor(x.astype(F32) * (1.0 / by)).astype(jnp.int32)
    r = x - q * by
    q = q + jnp.where(r >= by, 1, 0) - jnp.where(r < 0, 1, 0)
    return q, x - q * by


def inject(dims, extents, step, given, out, halo):
    levels, rows, cols = dims
    lat_cells, lon_cells = extents
    width = cols + LANES
    north_sign, south_sign = pole_signs()
    first_row, first_col = lax.axis_index("colat") * rows, lax.axis_index("lon") * cols
    at_top, at_bottom = first_row == 0, first_row + rows == lat_cells
    half = lon_cells // 2

    def located(ids):
        level, rest = divided(ids, lat_cells * lon_cells)
        row, col = divided(rest, lon_cells)

        def lane(c):
            x = c - first_col
            x = jnp.where(x < 0, x + lon_cells, x)
            x = jnp.where(x >= lon_cells, x - lon_cells, x)
            tail = x - lon_cells + cols + LANES
            tail = jnp.where(tail >= cols + LANES - EDGE, tail, -1)
            return jnp.where(x < cols + EDGE, x, tail)

        def code(r, count):
            inside = jnp.logical_and(r >= 0, r < count)
            return jnp.where(inside, r * levels + level, -1)

        north = 1 - jnp.where(at_top, row, first_row - 1 - row)
        south = jnp.where(at_bottom, lat_cells - 1 - row, row - first_row - rows)
        return (
            (code(row - first_row, rows), lane(col)),
            (code(north, 2), lane(jnp.where(at_top, col + half, col))),
            (code(south, 2), lane(jnp.where(at_bottom, col + half, col))),
        )

    def spread(place, value_rows, count):
        code, lane = place
        n = code.shape[1]
        hot_rows = lax.broadcasted_iota(jnp.int32, (count * levels, n), 0) == code
        hot = lax.broadcasted_iota(jnp.int32, (width, n), 0) == lane
        hot = jnp.where(hot, 1.0, 0.0).astype(jnp.bfloat16)
        out = []
        for value in value_rows:
            rest = jnp.where(hot_rows, value, 0.0)
            total = None
            for _ in range(3):
                part = rest.astype(jnp.bfloat16)
                rest = rest - part.astype(F32)
                term = lax.dot_general(
                    part, hot, (((1,), (1,)), ((), ())), preferred_element_type=F32
                )
                total = term if total is None else total + term
            out.append(total.reshape(count, levels, width))
        return out

    places = located(given[0:1, :].astype(jnp.int32))
    splaces = located(given[7:8, :LANES].astype(jnp.int32))
    values = [given[1 + 3 * step + c : 2 + 3 * step + c, :] for c in range(3)]
    svalues = [given[8 + step : 9 + step, :LANES]]
    regions = ((0, halo, rows, 1.0), (1, 0, halo, north_sign), (2, halo + rows, halo, south_sign))
    for where, at, count, sign in regions:
        if count:
            out[0, at : at + count] = spread(splaces[where], svalues, count)[0]
            for c, got in enumerate(spread(places[where], values, count)):
                signed = where and FIELD_SIGNS[c] < 0
                out[1 + c, at : at + count] = got * sign if signed else got


def first_inject_kernel(dims, extents, given, out, ap, cv):
    levels, rows, _ = dims
    lat_cells, lon_cells = extents
    first_row = lax.axis_index("colat") * rows
    inject(dims, extents, 0, given, out, 0)
    deep = rows + 2 * S_ROWS
    g = lax.broadcasted_iota(jnp.int32, (deep, LANES), 0) + (first_row - S_ROWS)
    sign = jnp.where(jnp.logical_or(g < 0, g >= lat_cells), -1.0, 1.0)
    g = jnp.where(g < 0, -1 - g, jnp.where(g >= lat_cells, 2 * lat_cells - 1 - g, g))
    angle = (g.astype(F32) + 0.5) * (math.pi / lat_cells)
    held = jnp.maximum(jnp.sin(angle), SIN_FLOOR)
    across = sign / (held * (24.0 * math.pi / lon_cells))
    cot = sign * jnp.cos(angle) / held
    ir = level_vectors(levels, LANES, (1.0 - R_INNER) / levels, math.pi / lat_cells)[0]
    for i in range(deep):
        ap[i] = ir * across[i : i + 1, :]
        cv[i] = ir * cot[i : i + 1, :]


def second_inject_kernel(dims, extents, given, out):
    inject(dims, extents, 1, given, out, 2)


def level_vectors(levels, width, dr, theta_step):
    k = lax.broadcasted_iota(jnp.int32, (levels, width), 0)
    ir = 1.0 / (R_INNER + (k.astype(F32) + 0.5) * dr)
    up = jnp.where(k < levels - 1, 0.5 / dr, 0.0).astype(F32)
    down = jnp.where(k > 0, 0.5 / dr, 0.0).astype(F32)
    return ir, ir * (8.0 / 12.0 / theta_step), ir * (1.0 / 12.0 / theta_step), up, down


def along_theta(ref, k, i, c1, c2):
    return c1 * (ref[k, i + 1] - ref[k, i - 1]) - c2 * (ref[k, i + 2] - ref[k, i - 2])


def along_phi(x):
    return 8.0 * (rolled(x, -1) - rolled(x, 1)) - (rolled(x, -2) - rolled(x, 2))


def along_r(x, up, down):
    return up * rolled(x, -1, 0) - down * rolled(x, 1, 0)


def forces(stress, f, i, vectors, ap, cv):
    ir, c1, c2, up, down = vectors
    k = f * 6
    tt, pp, rr, tp, tr, pr = (stress[k + n, i] for n in range(6))
    f_t = (
        along_theta(stress, k, i, c1, c2)
        + ap * along_phi(tp)
        + along_r(tr, up, down)
        + cv * (tt - pp)
        + 3.0 * (ir * tr)
    )
    f_p = (
        along_theta(stress, k + 3, i, c1, c2)
        + ap * along_phi(pp)
        + along_r(pr, up, down)
        + 2.0 * (cv * tp)
        + 3.0 * (ir * pr)
    )
    f_r = (
        along_theta(stress, k + 4, i, c1, c2)
        + ap * along_phi(pr)
        + along_r(rr, up, down)
        + ir * (2.0 * rr - tt - pp)
        + cv * tr
    )
    return f_t, f_p, f_r


def stress_steps(vel, f, i, vectors, ap, cv, lam, mu2, keep):
    ir, c1, c2, up, down = (v[:, :keep] for v in vectors)
    k = f * 3
    whole = tuple(vel[k + n, i] for n in range(3))
    v_t, v_p, v_r = (x[:, :keep] for x in whole)
    p_t, p_p, p_r = (along_phi(x)[:, :keep] for x in whole)

    def theta(n):
        return c1 * (vel[k + n, i + 1, :, :keep] - vel[k + n, i - 1, :, :keep]) - c2 * (
            vel[k + n, i + 2, :, :keep] - vel[k + n, i - 2, :, :keep]
        )

    ir_r = ir * v_r
    e_tt = theta(0) + ir_r
    e_pp = ap * p_p + cv * v_t + ir_r
    e_rr = along_r(v_r, up, down)
    e_tp = theta(1) - cv * v_p + ap * p_t
    e_tr = along_r(v_t, up, down) - ir * v_t + theta(2)
    e_pr = along_r(v_p, up, down) - ir * v_p + ap * p_r
    bulk = lam * (e_tt + e_pp + e_rr)
    half_mu = 0.5 * mu2
    return (
        bulk + mu2 * e_tt,
        bulk + mu2 * e_pp,
        bulk + mu2 * e_rr,
        half_mu * e_tp,
        half_mu * e_tr,
        half_mu * e_pr,
    )


def look_up(ids, tables):
    out = [jnp.full(ids.shape, table[0], F32) for table in tables]
    for n in range(1, tables[0].shape[0]):
        hit = ids == float(n)
        out = [jnp.where(hit, table[n], x) for table, x in zip(tables, out)]
    return out


def materials(ids, dt, tables):
    rho, lam, mu = look_up(ids, tables)
    return dt / rho, dt * lam, (2.0 * dt) * mu


def widened(x, width):
    return jnp.concatenate([x] * (width // LANES), axis=1)


def north_south(ref_a, ref_b, k):
    even = even_band()
    a, b = ref_a[k], ref_b[k]
    return jnp.where(even, b, a), jnp.where(even, a, b)


def velocity_kernel(
    dims, consts, state, ids, edge_a, edge_b, near_a, near_b, ap, cv, first, density,
    stress, vel, pay_a, pay_b, rho, id_side,
):
    levels, rows, cols = dims
    dr, theta_step, dt = consts
    width = cols + LANES
    signs = pole_signs()
    even = even_band()
    per = LANES // EDGE
    paired = {}

    def side_of(j):
        if j // per not in paired:
            paired[j // per] = paired_edges(edge_a, edge_b, j // per)
        return side_vector(paired[j // per], j % per)

    for f in range(2):
        for c in range(9):
            for r in range(rows):
                main = strided(state, (f * 9 + c) * levels * rows + r, levels, rows)
                side = side_of((f * 9 + c) * rows + r)
                if c < 3:
                    ref, k, i = vel, f * 3 + c, r
                else:
                    ref, k, i = stress, f * 6 + c - 3, r + S_ROWS
                ref[k, i, :, :cols] = main
                ref[k, i, :, cols:] = side
    for r in range(rows):
        main = strided(ids, r, levels, rows).astype(F32)
        side = side_of(18 * rows + r)
        id_side[r] = side
        rho[r, :, :cols] = dt / look_up(main, (density,))[0]
        rho[r, :, cols:] = dt / look_up(side, (density,))[0]
    for k, (f, c, d) in enumerate(NEAR):
        for main, i, sign in zip(
            north_south(near_a, near_b, k), (S_ROWS - d, S_ROWS + rows - 1 + d), signs
        ):
            if FIELD_SIGNS[c] < 0:
                main = main * sign
            stress[f * 6 + c - 3, i, :, :cols] = main
            stress[f * 6 + c - 3, i, :, cols:] = jnp.zeros((levels, LANES), F32)

    vectors = level_vectors(levels, width, dr, theta_step)

    def step(r, carry):
        i = r + S_ROWS
        scale = rho[r]
        row_ap, row_cv = widened(ap[i], width), widened(cv[i], width)
        for f in range(2):
            for c, force in enumerate(forces(stress, f, i, vectors, row_ap, row_cv)):
                new = vel[f * 3 + c, r] + scale * force
                if f == 1 or c == 2:
                    new = new + first[f * (1 + c), r]
                vel[f * 3 + c, r] = new
        return carry

    lax.fori_loop(0, rows, step, 0, unroll=8)

    tiles = cols // LANES
    plan, vectors_out = side_plan()
    for ref, bottom_side in ((pay_a, even), (pay_b, jnp.logical_not(even))):

        def facing(d):
            return jnp.where(bottom_side, rows - d, d - 1)

        for k, (f, c, d) in enumerate(VEL):
            for t in range(tiles):
                at = slice(t * LANES, (t + 1) * LANES)
                ref[k * tiles + t] = vel[f * 3 + c, facing(d), :, at]
        packed, lanes = [None] * vectors_out, lane_iota((levels, LANES))
        for (kind, f, c, d), (v, lane, wide) in plan.items():
            if kind == "v":
                x = vel[f * 3 + c, facing(d), :, cols:]
            elif kind == "s":
                x = stress[f * 6 + c - 3, facing(d) + S_ROWS, :, cols:]
            else:
                x = id_side[facing(d)]
            x = rolled(x, lane + wide // 2)
            packed[v] = x if packed[v] is None else jnp.where(lanes >= lane, x, packed[v])
        for v, x in enumerate(packed):
            ref[len(VEL) * tiles + v] = x


def fill_kernel(
    dims, consts, stress, vel, ids, id_edge_a, id_edge_b, far_a, far_b, second, ap, cv,
    density, lame, shear, halo, mats, inner_stress, inner_vel, inner_density,
):
    levels, rows, cols = dims
    dr, theta_step, dt = consts
    width = cols + LANES
    signs = pole_signs()
    tables = density, lame, shear
    per = LANES // EDGE
    paired = {}

    for k, (f, c, d) in enumerate(FAR):
        for main, i, sign in zip(
            north_south(far_a, far_b, k), (S_ROWS - d, S_ROWS - 1 + d), signs
        ):
            halo[f * 6 + c - 3, i] = main * sign if FIELD_SIGNS[c] < 0 else main
    for f, c, d in NEAR:
        k = f * 6 + c - 3
        halo[k, S_ROWS - d] = stress[k, S_ROWS - d, :, :cols]
        halo[k, S_ROWS - 1 + d] = stress[k, S_ROWS + rows - 1 + d, :, :cols]

    def material(i, x, at):
        for n, value in enumerate(materials(x, dt, tables)):
            mats[n, i, :, at] = value

    main, side = slice(0, cols), slice(cols, cols + LANES)
    for r in range(rows):
        material(r + S_ROWS, strided(ids, r, levels, rows).astype(F32), main)
        v, slot = divmod(18 * rows + r, per)
        if v not in paired:
            paired[v] = paired_edges(id_edge_a, id_edge_b, v)
        material(r + S_ROWS, side_vector(paired[v], slot), side)
    for d in range(1, S_ROWS + 1):
        north, south = north_south(far_a, far_b, FAR_IDS + d - 1)
        material(S_ROWS - d, north, main)
        material(S_ROWS + rows - 1 + d, south, main)

    vectors = level_vectors(levels, width, dr, theta_step)

    def inner_first(r, carry):
        i = r + S_ROWS
        row_ap, row_cv = widened(ap[i], width), widened(cv[i], width)
        for f in range(2):
            new = stress_steps(vel, f, r, vectors, row_ap, row_cv, mats[1, i], mats[2, i], width)
            for n in range(6):
                inner_stress[f * 6 + n, r - INNER] = stress[f * 6 + n, i] + new[n]
        return carry

    lax.fori_loop(INNER, rows - INNER, inner_first, 0, unroll=4)

    def inner_second(r, carry):
        i = r + S_ROWS
        at = r - INNER - 2
        row_ap, row_cv = widened(ap[i], width), widened(cv[i], width)
        products = [vel[c, r, :, :cols] * vel[3 + c, r, :, :cols] for c in range(3)]
        fresh = []
        for f in range(2):
            steps = forces(inner_stress, f, r - INNER, vectors, row_ap, row_cv)
            for c, force in enumerate(steps):
                new = vel[f * 3 + c, r] + mats[0, i] * force
                if f == 1 or c == 2:
                    new = new + second[f * (1 + c), r + 2]
                inner_vel[f * 3 + c, at] = new
                fresh.append(new[:, :cols])
        products += [fresh[c] * fresh[3 + c] for c in range(3)]
        inner_density[at] = sum(products[1:], products[0])
        return carry

    lax.fori_loop(INNER + 2, rows - INNER - 2, inner_second, 0, unroll=4)


def final_kernel(
    dims, consts, vel_in, stress_in, halo, got_a, got_b, mats_in, second, ap, cv,
    inner_stress, inner_vel, inner_density, density_t, lame_t, shear_t,
    fwd_out, adj_out, density_out, vel, stress, mats, fwd, adj, density, sems,
):
    levels, rows, cols = dims
    dr, theta_step, dt = consts
    width = cols + LANES
    signs = pole_signs()
    tiles = cols // LANES
    side_at = slice(cols, width)
    plan, _ = side_plan()
    lanes_shape = (levels, LANES)

    def sides(kind, f, c, d):
        if (kind, f, c, d) not in plan:
            return (jnp.zeros(lanes_shape, F32),) * 2
        v, lane, wide = plan[kind, f, c, d]
        got = north_south(got_a, got_b, len(VEL) * tiles + v)
        return tuple(rolled(x, -lane - wide // 2) for x in got)

    for k, (f, c, d) in enumerate(VEL):
        flip = FIELD_SIGNS[c] < 0
        for t in range(tiles):
            at = slice(t * LANES, (t + 1) * LANES)
            north, south = north_south(got_a, got_b, k * tiles + t)
            vel[f * 3 + c, V_ROWS - d, :, at] = north * signs[0] if flip else north
            vel[f * 3 + c, V_ROWS + rows - 1 + d, :, at] = south * signs[1] if flip else south
        at = V_ROWS - d, V_ROWS + rows - 1 + d
        for x, i, sign in zip(sides("v", f, c, d), at, signs):
            vel[f * 3 + c, i, :, side_at] = x * sign if flip else x
    for f, c, d in NEAR + FAR:
        n = f * 6 + c - 3
        for x, i, i_main, sign in zip(
            sides("s", f, c, d),
            (S_ROWS - d, S_ROWS + rows - 1 + d),
            (S_ROWS - d, S_ROWS - 1 + d),
            signs,
        ):
            stress[n, i, :, side_at] = x * sign if FIELD_SIGNS[c] < 0 else x
            stress[n, i, :, :cols] = halo[n, i_main]
    for d in range(1, S_ROWS + 1):
        for x, i in zip(sides("i", 0, 0, d), (S_ROWS - d, S_ROWS + rows - 1 + d)):
            for n, value in enumerate(materials(x, dt, (density_t, lame_t, shear_t))):
                mats[n, i, :, side_at] = value
                mats[n, i, :, :cols] = mats_in[n, i, :, :cols]
    for n in range(3):
        for r in range(rows):
            mats[n, S_ROWS + r] = mats_in[n, S_ROWS + r]
    for k in range(6):
        for r in range(rows):
            vel[k, V_ROWS + r] = vel_in[k, r]
    for n in range(12):
        for r in range(INNER, rows - INNER):
            stress[n, S_ROWS + r] = inner_stress[n, r - INNER]

    vectors = level_vectors(levels, width, dr, theta_step)
    c1, c2 = vectors[1][:, :LANES], vectors[2][:, :LANES]

    def add_side(k, r, value):
        scale = mats[0, S_ROWS + r, :, side_at]
        vel[k, V_ROWS + r, :, side_at] = vel[k, V_ROWS + r, :, side_at] + scale * value

    for f in range(2):
        for c in range(3):
            k, n = f * 3 + c, f * 6 + CROSS[c] - 3
            n1, n2 = (stress[n, S_ROWS - d, :, side_at] for d in (1, 2))
            s1, s2 = (stress[n, S_ROWS + rows - 1 + d, :, side_at] for d in (1, 2))
            o1, o2 = (stress_in[n, S_ROWS + d, :, side_at] for d in (0, 1))
            u1, u2 = (stress_in[n, S_ROWS + rows - d, :, side_at] for d in (1, 2))
            add_side(k, 0, c2 * n2 - c1 * n1)
            add_side(k, 1, c2 * n1)
            add_side(k, rows - 1, c1 * s1 - c2 * s2)
            add_side(k, rows - 2, -(c2 * s1))
            add_side(k, -1, c1 * o1 - c2 * o2)
            add_side(k, -2, -(c2 * o1))
            add_side(k, rows, c2 * u2 - c1 * u1)
            add_side(k, rows + 1, c2 * u1)

    def first_stress(before, i, carry):
        row_ap, row_cv = widened(ap[i], width), widened(cv[i], width)
        lam, mu2 = mats[1, i], mats[2, i]
        for f in range(2):
            new = stress_steps(
                vel, f, i + V_ROWS - S_ROWS, vectors, row_ap, row_cv, lam, mu2, width
            )
            for n in range(6):
                stress[f * 6 + n, i] = before[f * 6 + n, i] + new[n]
        return carry

    inner = S_ROWS + rows
    lax.fori_loop(0, S_ROWS, functools.partial(first_stress, stress), 0, unroll=4)
    outer = functools.partial(first_stress, stress_in)
    lax.fori_loop(S_ROWS, S_ROWS + INNER, outer, 0, unroll=4)
    lax.fori_loop(inner - INNER, inner, outer, 0, unroll=4)
    lax.fori_loop(inner, inner + S_ROWS, functools.partial(first_stress, stress), 0, unroll=4)

    def second_velocity(own, r, carry):
        i = r + S_ROWS - 2
        j = r + V_ROWS - 2
        row_ap, row_cv = widened(ap[i], width), widened(cv[i], width)
        scale = mats[0, i]
        fresh, products = [], []
        if own:
            for c in range(3):
                products.append(vel[c, j, :, :cols] * vel[3 + c, j, :, :cols])
        for f in range(2):
            for c, force in enumerate(forces(stress, f, i, vectors, row_ap, row_cv)):
                new = vel[f * 3 + c, j] + scale * force
                if f == 1 or c == 2:
                    new = new + second[f * (1 + c), r]
                vel[f * 3 + c, j] = new
                fresh.append(new[:, :cols])
        if own:
            for c in range(3):
                products.append(fresh[c] * fresh[3 + c])
            density[pl.ds(r - 2, levels, stride=rows), :] = sum(products[1:], products[0])
            for f in range(2):
                for c in range(3):
                    at = c * levels * rows + r - 2
                    (fwd, adj)[f][pl.ds(at, levels, stride=rows), :] = fresh[f * 3 + c]
        return carry

    reach = INNER + 2
    own = functools.partial(second_velocity, True)
    lax.fori_loop(0, 2, functools.partial(second_velocity, False), 0, unroll=2)
    lax.fori_loop(2, 2 + reach, own, 0, unroll=6)
    lax.fori_loop(2 + rows - reach, 2 + rows, own, 0, unroll=6)
    lax.fori_loop(rows + 2, rows + 4, functools.partial(second_velocity, False), 0, unroll=2)
    for r in range(reach, rows - reach):
        density[pl.ds(r, levels, stride=rows), :] = inner_density[r - reach]
        for k in range(6):
            x = inner_vel[k, r - reach]
            vel[k, V_ROWS + r] = x
            at = k % 3 * levels * rows + r
            (fwd, adj)[k // 3][pl.ds(at, levels, stride=rows), :] = x[:, :cols]

    split = 3 * levels * rows
    early, late = pl.ds(0, split), pl.ds(split, 6 * levels * rows)
    copies = [
        pltpu.make_async_copy(fwd.at[early], fwd_out.at[early], sems.at[0]),
        pltpu.make_async_copy(adj.at[early], adj_out.at[early], sems.at[1]),
        pltpu.make_async_copy(density, density_out, sems.at[2]),
    ]
    for copy in copies:
        copy.start()

    def second_stress(r, carry):
        i = r + S_ROWS
        row_ap, row_cv = widened(ap[i], cols), widened(cv[i], cols)
        lam, mu2 = mats[1, i, :, :cols], mats[2, i, :, :cols]
        for f in range(2):
            new = stress_steps(vel, f, r + V_ROWS, vectors, row_ap, row_cv, lam, mu2, cols)
            for n in range(6):
                at = (3 + n) * levels * rows + r
                (fwd, adj)[f][pl.ds(at, levels, stride=rows), :] = (
                    stress[f * 6 + n, i, :, :cols] + new[n]
                )
        return carry

    lax.fori_loop(0, rows, second_stress, 0, unroll=8)
    copies += [
        pltpu.make_async_copy(fwd.at[late], fwd_out.at[late], sems.at[3]),
        pltpu.make_async_copy(adj.at[late], adj_out.at[late], sems.at[4]),
    ]
    for copy in copies[3:]:
        copy.start()
    for copy in copies:
        copy.wait()


def swap_tiles(x, first):
    count = lax.axis_size("lon")
    to = {i: (i + (1 if (i % 2 == 0) == first else -1)) % count for i in range(count)}
    return lax.ppermute(x, "lon", list(to.items()))


def swap_bands(x, first):
    bands, count = lax.axis_size("colat"), lax.axis_size("lon")
    pairs = []
    for lon in range(count):
        for band in range(bands):
            to_band, to_lon = band + (1 if (band % 2 == 0) == first else -1), lon
            if to_band < 0 or to_band >= bands:
                to_band, to_lon = band, (lon + count // 2) % count
            pairs.append((lon * bands + band, to_lon * bands + to_band))
    return lax.ppermute(x, ("lon", "colat"), pairs)


def call(kernel, out_shapes, specs, cost=0, out=None, **more):
    return pl.pallas_call(
        kernel,
        out_shape=out_shapes,
        in_specs=specs,
        out_specs=jax.tree.map(lambda _: out or vmem(), out_shapes),
        cost_estimate=pl.CostEstimate(flops=cost, bytes_accessed=cost, transcendentals=0),
        compiler_params=pltpu.CompilerParams(vmem_limit_bytes=16 * 2**20),
        **more,
    )


def on_device(
    forward_state, adjoint_state, layer_ids, density_table, lame_table, shear_table,
    source_cells, source_wavelet, receiver_cells, receiver_residual,
):
    dims = levels, rows, cols = layer_ids.shape
    lat_cells = rows * lax.axis_size("colat")
    lon_cells = cols * lax.axis_size("lon")
    dt = COURANT * SIN_FLOOR * R_INNER * (2.0 * math.pi / lon_cells) / 1.6
    consts = ((1.0 - R_INNER) / levels, math.pi / lat_cells, dt)
    width = cols + LANES
    tiles = cols // LANES

    def shape(*dims):
        return jax.ShapeDtypeStruct(dims, F32)

    parts = forward_state, adjoint_state
    state = jnp.concatenate([x.reshape(-1, rows, cols) for x in parts]).reshape(-1, cols)
    ids = layer_ids.reshape(levels * rows, cols)

    edges = shape(pieces(19 * rows, EDGE), levels, LANES)
    near = shape(len(NEAR), levels, cols)
    far = shape(len(FAR) + S_ROWS, levels, cols)
    edge_a, edge_b, near_a, near_b, far_a, far_b = call(
        functools.partial(pack_kernel, dims),
        [edges, edges, near, near, far, far],
        [vmem()] * 2,
        cost=10**6,
    )(state, ids)
    near_b = swap_bands(near_b, False)
    near_a = swap_bands(near_a, True)
    edge_b = swap_tiles(edge_b, False)
    edge_a = swap_tiles(edge_a, True)
    far_b = swap_bands(far_b, False)
    far_a = swap_bands(far_a, True)

    deep = shape(rows + 2 * S_ROWS, levels, LANES)
    count = max(LANES, receiver_cells.shape[0])

    def lines(x):
        x = x.astype(F32).reshape(-1, x.shape[-1])
        return jnp.pad(x, ((0, 0), (0, count - x.shape[1])))

    given = jnp.concatenate(
        [lines(x) for x in (receiver_cells, receiver_residual, source_cells, source_wavelet)]
    )
    extents = lat_cells, lon_cells
    first, ap, cv = call(
        functools.partial(first_inject_kernel, dims, extents),
        [shape(4, rows, levels, width), deep, deep],
        [vmem()],
        cost=10**8,
    )(given)

    payload = shape(len(VEL) * tiles + side_plan()[1], levels, LANES)
    stress_shape = shape(12, rows + 2 * S_ROWS, levels, width)
    mats_shape = shape(3, rows + 2 * S_ROWS, levels, width)
    stress, vel, pay_a, pay_b = call(
        functools.partial(velocity_kernel, dims, consts),
        [stress_shape, shape(6, rows, levels, width), payload, payload],
        [vmem()] * 9 + [smem()],
        cost=10**7,
        scratch_shapes=[
            pltpu.VMEM((rows, levels, width), F32),
            pltpu.VMEM((rows, levels, LANES), F32),
        ],
    )(state, ids, edge_a, edge_b, near_a, near_b, ap, cv, first, density_table)
    got_b, got_a = swap_bands(pay_b, False), swap_bands(pay_a, True)

    second = call(
        functools.partial(second_inject_kernel, dims, extents),
        shape(4, rows + 4, levels, width),
        [vmem()],
        cost=10**8,
    )(given)
    halo, mats, inner_stress, inner_vel, inner_density = call(
        functools.partial(fill_kernel, dims, consts),
        [
            shape(12, 2 * S_ROWS, levels, cols),
            mats_shape,
            shape(12, rows - 2 * INNER, levels, width),
            shape(6, rows - 2 * INNER - 4, levels, width),
            shape(rows - 2 * INNER - 4, levels, cols),
        ],
        [vmem()] * 10 + [smem()] * 3,
        cost=10**8,
    )(
        stress, vel, ids, edge_a, edge_b, far_a, far_b, second, ap, cv,
        density_table, lame_table, shear_table,
    )

    flat = (9 * levels * rows, cols), (9 * levels * rows, cols), (levels * rows, cols)
    fwd, adj, density = call(
        functools.partial(final_kernel, dims, consts),
        [shape(*x) for x in flat],
        [vmem()] * 12 + [smem()] * 3,
        cost=10**8,
        out=pl.BlockSpec(memory_space=pltpu.HBM),
        scratch_shapes=[
            pltpu.VMEM((6, rows + 2 * V_ROWS, levels, width), F32),
            pltpu.VMEM(stress_shape.shape, F32),
            pltpu.VMEM(mats_shape.shape, F32),
        ]
        + [pltpu.VMEM(x, F32) for x in flat]
        + [pltpu.SemaphoreType.DMA((5,))],
    )(
        vel, stress, halo, got_a, got_b, mats, second, ap, cv,
        inner_stress, inner_vel, inner_density, density_table, lame_table, shear_table,
    )
    return (
        fwd.reshape(forward_state.shape),
        adj.reshape(adjoint_state.shape),
        density.reshape(layer_ids.shape),
    )


def solution(mesh):
    return jax.shard_map(
        on_device,
        mesh=mesh,
        in_specs=(
            P(None, None, "colat", "lon"),
            P(None, None, "colat", "lon"),
            P(None, "colat", "lon"),
        )
        + (P(),) * 7,
        out_specs=(
            P(None, None, "colat", "lon"),
            P(None, None, "colat", "lon"),
            P(None, "colat", "lon"),
        ),
        check_vma=False,
    )
```

```python
import functools
import math

import jax
import jax.numpy as jnp
from jax import lax
from jax.experimental import pallas as pl
from jax.experimental.pallas import tpu as pltpu
from jax.sharding import PartitionSpec as P

R_INNER = 0.55
COURANT = 0.3
SIN_FLOOR = 0.25
FIELD_SIGNS = (-1, -1, 1, 1, 1, 1, 1, -1, -1)
CROSS = (3, 6, 7)
OTHER = (4, 5, 8)
EDGE = 8
LANES = 128
V_ROWS = 6
S_ROWS = 4
INNER = 4
F32 = jnp.float32


NEAR = tuple((f, c, d) for f in range(2) for c in CROSS for d in (1, 2))
FAR = tuple((f, c, d) for f in range(2) for c in OTHER for d in (1, 2)) + tuple(
    (f, c, d) for f in range(2) for c in CROSS for d in (3, 4)
)
FAR_IDS = len(FAR)
VEL = tuple((f, c, d) for f in range(2) for c in range(3) for d in range(1, V_ROWS + 1))


def vmem():
    return pl.BlockSpec(memory_space=pltpu.VMEM)


def smem():
    return pl.BlockSpec(memory_space=pltpu.SMEM)


def lane_iota(shape):
    return lax.broadcasted_iota(jnp.int32, shape, 1)


def rolled(x, shift, axis=1):
    size = x.shape[axis]
    shift = shift % size
    return x if shift == 0 else pltpu.roll(x, shift, axis)


def side_plan():
    wide = [("v", f, c, 1) for f in range(2) for c in range(3)]
    wide += [("s",) + entry for entry in NEAR] + [("i", 0, 0, 1)]
    slim = [("v", f, c, d) for f, c, d in VEL if 1 < d < V_ROWS]
    slim += [("s",) + entry for entry in FAR if entry[2] < S_ROWS] + [("i", 0, 0, 2), ("i", 0, 0, 3)]
    plan, lane = {}, 0
    for width, entries in ((2 * EDGE, wide), (EDGE, slim)):
        for entry in entries:
            plan[entry] = (lane // LANES, lane % LANES, width)
            lane += width
    return plan, -(-lane // LANES)


def pieces(count, width):
    per = LANES // width
    return -(-count // per)


def paired_edges(edge_a, edge_b, v):
    a, b = edge_a[v], edge_b[v]
    even = even_tile()
    after, before = jnp.where(even, a, b), jnp.where(even, b, a)
    odd_lane = lax.rem(lane_iota(a.shape) // EDGE, 2) == 1
    return jnp.where(odd_lane, before, after), jnp.where(odd_lane, after, before)


def side_vector(paired, slot):
    return rolled(paired[slot % 2], -slot * EDGE)


def even_band():
    return lax.rem(lax.axis_index("colat"), 2) == 0


def even_tile():
    return lax.rem(lax.axis_index("lon"), 2) == 0


def pole_signs():
    band, last = lax.axis_index("colat"), lax.axis_size("colat") - 1
    north = jnp.where(band == 0, -1.0, 1.0).astype(F32)
    south = jnp.where(band == last, -1.0, 1.0).astype(F32)
    return north, south


def strided(ref, first, levels, rows):
    return ref[pl.ds(first, levels, stride=rows), :]


def pack_kernel(dims, state, ids, edge_a, edge_b, near_a, near_b, far_a, far_b):
    levels, rows, cols = dims
    even = even_band()

    def row(f, c, r):
        return strided(state, (f * 9 + c) * levels * rows + r, levels, rows)

    def id_row(r):
        return strided(ids, r, levels, rows).astype(F32)

    def put(ref_a, ref_b, k, get, d):
        top, bottom = get(d - 1), get(rows - d)
        ref_a[k], ref_b[k] = jnp.where(even, bottom, top), jnp.where(even, top, bottom)

    for k, (f, c, d) in enumerate(NEAR):
        put(near_a, near_b, k, functools.partial(row, f, c), d)
    for k, (f, c, d) in enumerate(FAR):
        put(far_a, far_b, k, functools.partial(row, f, c), d)
    for d in range(1, S_ROWS + 1):
        put(far_a, far_b, FAR_IDS + d - 1, id_row, d)

    per = LANES // EDGE
    edges = [functools.partial(row, f, c, r) for f in range(2) for c in range(9) for r in range(rows)]
    edges += [functools.partial(id_row, r) for r in range(rows)]
    lane = lane_iota((levels, LANES))
    swapped = jnp.logical_not(even_tile())
    for v in range(edge_a.shape[0]):
        east = west = None
        for slot, get in reversed(list(enumerate(edges[v * per : (v + 1) * per]))):
            x = get()
            last = rolled(x[:, cols - LANES :], slot * EDGE)
            first = last if cols == LANES else rolled(x[:, :LANES], slot * EDGE)
            if east is None:
                east, west = last, first
            else:
                west = jnp.where(lane < (slot + 1) * EDGE, first, west)
                if slot:
                    east = jnp.where(lane < slot * EDGE, last, east)
                else:
                    east = jnp.where(lane < LANES - EDGE, east, last)
        edge_a[v] = jnp.where(swapped, west, east)
        edge_b[v] = jnp.where(swapped, east, west)


def divided(x, by):
    q = jnp.floor(x.astype(F32) * (1.0 / by)).astype(jnp.int32)
    r = x - q * by
    q = q + jnp.where(r >= by, 1, 0) - jnp.where(r < 0, 1, 0)
    return q, x - q * by


def inject_kernel(dims, extents, given, first, second):
    levels, rows, cols = dims
    lat_cells, lon_cells = extents
    width = cols + LANES
    signs = (1.0,) + pole_signs()
    first_row, first_col = lax.axis_index("colat") * rows, lax.axis_index("lon") * cols
    at_top, at_bottom = first_row == 0, first_row + rows == lat_cells
    half = lon_cells // 2

    def located(ids):
        level, rest = divided(ids, lat_cells * lon_cells)
        row, col = divided(rest, lon_cells)

        def lane(c):
            x = c - first_col
            x = jnp.where(x < 0, x + lon_cells, x)
            x = jnp.where(x >= lon_cells, x - lon_cells, x)
            tail = x - lon_cells + cols + LANES
            tail = jnp.where(tail >= cols + LANES - EDGE, tail, -1)
            return jnp.where(x < cols + EDGE, x, tail)

        def code(r, count):
            inside = jnp.logical_and(r >= 0, r < count)
            return jnp.where(inside, r * levels + level, -1)

        north = V_ROWS - 1 - jnp.where(at_top, row, first_row - 1 - row)
        south = jnp.where(at_bottom, lat_cells - 1 - row, row - first_row - rows)
        return (
            (code(row - first_row, rows), lane(col)),
            (code(north, V_ROWS), lane(jnp.where(at_top, col + half, col))),
            (code(south, V_ROWS), lane(jnp.where(at_bottom, col + half, col))),
        )

    def parts(value):
        out, rest = [], value
        for _ in range(3):
            part = rest.astype(jnp.bfloat16)
            out.append(part)
            rest = rest - part.astype(F32)
        return out

    def hot(ids, size):
        same = lax.broadcasted_iota(jnp.int32, (size, ids.shape[1]), 0) == ids
        return jnp.where(same, 1.0, 0.0).astype(jnp.bfloat16)

    def line(n, size):
        return given[n : n + 1, :size]

    places = located(line(0, None).astype(jnp.int32))
    splaces = located(line(7, LANES).astype(jnp.int32))
    regions = ((V_ROWS, rows), (0, V_ROWS), (V_ROWS + rows, V_ROWS))
    receivers = [(s, 1 + c, parts(line(1 + 3 * s + c, None))) for s in range(2) for c in range(3)]
    sources = [(s, 0, parts(line(8 + s, LANES))) for s in range(2)]
    for n, (at, count) in enumerate(regions):
        size = count * levels
        for place, todo in ((places[n], receivers), (splaces[n], sources)):
            on_row, on_lane = hot(place[0], size), hot(place[1], width)
            stacked = jnp.concatenate([on_row * part for _, _, three in todo for part in three])
            spread = lax.dot_general(
                stacked, on_lane, (((1,), (1,)), ((), ())), preferred_element_type=F32
            )
            for m, (s, k, _) in enumerate(todo):
                rest = [spread[(3 * m + p) * size : (3 * m + p + 1) * size] for p in range(3)]
                total = rest[0] + rest[1] + rest[2]
                if n and k and FIELD_SIGNS[k - 1] < 0:
                    total = total * signs[n]
                (first, second)[s][k, at : at + count] = total.reshape(count, levels, width)


def geometry(dims, extents):
    levels, rows, _ = dims
    lat_cells, lon_cells = extents
    first_row = lax.axis_index("colat") * rows
    g = first_row + jnp.arange(-S_ROWS, rows + S_ROWS, dtype=jnp.int32)
    sign = jnp.where(jnp.logical_or(g < 0, g >= lat_cells), -1.0, 1.0)
    g = jnp.where(g < 0, -1 - g, jnp.where(g >= lat_cells, 2 * lat_cells - 1 - g, g))
    angle = (g.astype(F32) + 0.5) * (math.pi / lat_cells)
    held = jnp.maximum(jnp.sin(angle), SIN_FLOOR)
    pair = sign / (held * (24.0 * math.pi / lon_cells)), sign * jnp.cos(angle) / held
    pair = lax.optimization_barrier(pair)
    k = jnp.arange(levels, dtype=F32)
    ir = 1.0 / (R_INNER + (k + 0.5) * ((1.0 - R_INNER) / levels))
    shape = g.shape[0], levels, LANES
    return tuple(
        jnp.broadcast_to(x[:, None, None] * ir[None, :, None], shape) for x in pair
    )


def level_vectors(levels, width, dr, theta_step):
    k = lax.broadcasted_iota(jnp.int32, (levels, width), 0)
    ir = 1.0 / (R_INNER + (k.astype(F32) + 0.5) * dr)
    up = jnp.where(k < levels - 1, 0.5 / dr, 0.0).astype(F32)
    down = jnp.where(k > 0, 0.5 / dr, 0.0).astype(F32)
    return ir, ir * (8.0 / 12.0 / theta_step), ir * (1.0 / 12.0 / theta_step), up, down


def along_theta(ref, k, i, c1, c2):
    return c1 * (ref[k, i + 1] - ref[k, i - 1]) - c2 * (ref[k, i + 2] - ref[k, i - 2])


def along_phi(x):
    return 8.0 * (rolled(x, -1) - rolled(x, 1)) - (rolled(x, -2) - rolled(x, 2))


def along_r(x, up, down):
    return up * rolled(x, -1, 0) - down * rolled(x, 1, 0)


def forces(stress, f, i, vectors, ap, cv):
    ir, c1, c2, up, down = vectors
    k = f * 6
    tt, pp, rr, tp, tr, pr = (stress[k + n, i] for n in range(6))
    f_t = (
        along_theta(stress, k, i, c1, c2)
        + ap * along_phi(tp)
        + along_r(tr, up, down)
        + cv * (tt - pp)
        + 3.0 * (ir * tr)
    )
    f_p = (
        along_theta(stress, k + 3, i, c1, c2)
        + ap * along_phi(pp)
        + along_r(pr, up, down)
        + 2.0 * (cv * tp)
        + 3.0 * (ir * pr)
    )
    f_r = (
        along_theta(stress, k + 4, i, c1, c2)
        + ap * along_phi(pr)
        + along_r(rr, up, down)
        + ir * (2.0 * rr - tt - pp)
        + cv * tr
    )
    return f_t, f_p, f_r


def stress_steps(vel, f, i, vectors, ap, cv, lam, mu2, keep):
    ir, c1, c2, up, down = (v[:, :keep] for v in vectors)
    k = f * 3
    whole = tuple(vel[k + n, i] for n in range(3))
    v_t, v_p, v_r = (x[:, :keep] for x in whole)
    p_t, p_p, p_r = (along_phi(x)[:, :keep] for x in whole)

    def theta(n):
        return c1 * (vel[k + n, i + 1, :, :keep] - vel[k + n, i - 1, :, :keep]) - c2 * (
            vel[k + n, i + 2, :, :keep] - vel[k + n, i - 2, :, :keep]
        )

    ir_r = ir * v_r
    e_tt = theta(0) + ir_r
    e_pp = ap * p_p + cv * v_t + ir_r
    e_rr = along_r(v_r, up, down)
    e_tp = theta(1) - cv * v_p + ap * p_t
    e_tr = along_r(v_t, up, down) - ir * v_t + theta(2)
    e_pr = along_r(v_p, up, down) - ir * v_p + ap * p_r
    bulk = lam * (e_tt + e_pp + e_rr)
    half_mu = 0.5 * mu2
    return (
        bulk + mu2 * e_tt,
        bulk + mu2 * e_pp,
        bulk + mu2 * e_rr,
        half_mu * e_tp,
        half_mu * e_tr,
        half_mu * e_pr,
    )


def look_up(ids, tables):
    out = [jnp.full(ids.shape, table[0], F32) for table in tables]
    for n in range(1, tables[0].shape[0]):
        hit = ids == float(n)
        out = [jnp.where(hit, table[n], x) for table, x in zip(tables, out)]
    return out


def materials(ids, dt, tables):
    rho, lam, mu = look_up(ids, tables)
    return dt / rho, dt * lam, (2.0 * dt) * mu


def widened(x, width):
    return jnp.concatenate([x] * (width // LANES), axis=1)


def north_south(ref_a, ref_b, k):
    even = even_band()
    a, b = ref_a[k], ref_b[k]
    return jnp.where(even, b, a), jnp.where(even, a, b)


def velocity_kernel(
    dims, consts, state, ids, edge_a, edge_b, near_a, near_b, ap, cv, given, density,
    stress, vel, rho, id_side, pay_b,
):
    levels, rows, cols = dims
    _, _, dt = consts
    signs = pole_signs()
    per = LANES // EDGE
    paired = {}

    def side_of(j):
        if j // per not in paired:
            paired[j // per] = paired_edges(edge_a, edge_b, j // per)
        return side_vector(paired[j // per], j % per)

    for f in range(2):
        for c in range(9):
            for r in range(rows):
                main = strided(state, (f * 9 + c) * levels * rows + r, levels, rows)
                side = side_of((f * 9 + c) * rows + r)
                if c < 3:
                    ref, k, i = vel, f * 3 + c, r
                else:
                    ref, k, i = stress, f * 6 + c - 3, r + S_ROWS
                ref[k, i, :, :cols] = main
                ref[k, i, :, cols:] = side
    for r in range(rows):
        main = strided(ids, r, levels, rows).astype(F32)
        side = side_of(18 * rows + r)
        id_side[r] = side
        rho[r, :, :cols] = dt / look_up(main, (density,))[0]
        rho[r, :, cols:] = dt / look_up(side, (density,))[0]
    for k, (f, c, d) in enumerate(NEAR):
        for main, i, sign in zip(
            north_south(near_a, near_b, k), (S_ROWS - d, S_ROWS + rows - 1 + d), signs
        ):
            if FIELD_SIGNS[c] < 0:
                main = main * sign
            stress[f * 6 + c - 3, i, :, :cols] = main
            stress[f * 6 + c - 3, i, :, cols:] = jnp.zeros((levels, LANES), F32)

    base = jnp.where(even_band(), 0, rows - V_ROWS)
    step = velocity_step(dims, consts, stress, vel, vel, rho, ap, cv)
    lax.fori_loop(0, V_ROWS, lambda q, carry: step(base + q, carry), 0, unroll=V_ROWS)
    payload(dims, jnp.logical_not(even_band()), stress, vel, id_side, pay_b)


def rest_kernel(dims, consts, stress, vel_in, rho, id_side, ap, cv, vel, pay_a):
    _, rows, _ = dims
    done = jnp.where(even_band(), 0, rows - V_ROWS)
    base = jnp.where(even_band(), V_ROWS, 0)
    for q in range(V_ROWS):
        for k in range(6):
            vel[k, done + q] = vel_in[k, done + q]
    step = velocity_step(dims, consts, stress, vel_in, vel, rho, ap, cv)
    lax.fori_loop(0, rows - V_ROWS, lambda q, carry: step(base + q, carry), 0, unroll=5)
    payload(dims, even_band(), stress, vel, id_side, pay_a)


def velocity_step(dims, consts, stress, before, after, rho, ap, cv):
    levels, _, cols = dims
    dr, theta_step, _ = consts
    width = cols + LANES
    vectors = level_vectors(levels, width, dr, theta_step)

    def step(r, carry):
        i = r + S_ROWS
        scale = rho[r]
        row_ap, row_cv = widened(ap[i], width), widened(cv[i], width)
        for f in range(2):
            for c, force in enumerate(forces(stress, f, i, vectors, row_ap, row_cv)):
                after[f * 3 + c, r] = before[f * 3 + c, r] + scale * force
        return carry

    return step


def payload(dims, bottom_side, stress, vel, id_side, ref):
    levels, rows, cols = dims
    tiles = cols // LANES
    plan, vectors_out = side_plan()

    def facing(d):
        return jnp.where(bottom_side, rows - d, d - 1)

    for k, (f, c, d) in enumerate(VEL):
        for t in range(tiles):
            at = slice(t * LANES, (t + 1) * LANES)
            ref[k * tiles + t] = vel[f * 3 + c, facing(d), :, at]
    packed, lanes = [None] * vectors_out, lane_iota((levels, LANES))
    for (kind, f, c, d), (v, lane, wide) in plan.items():
        if kind == "v":
            x = vel[f * 3 + c, facing(d), :, cols:]
        elif kind == "s":
            x = stress[f * 6 + c - 3, facing(d) + S_ROWS, :, cols:]
        else:
            x = id_side[facing(d)]
        x = rolled(x, lane + wide // 2)
        packed[v] = x if packed[v] is None else jnp.where(lanes >= lane, x, packed[v])
    for v, x in enumerate(packed):
        ref[len(VEL) * tiles + v] = x


def fill_kernel(
    dims, consts, stress, vel_in, ids, id_edge_a, id_edge_b, far_a, far_b, first, second, ap, cv,
    density, lame, shear, halo, mats, vel, inner_stress, inner_vel, inner_density,
):
    levels, rows, cols = dims
    dr, theta_step, dt = consts
    width = cols + LANES
    signs = pole_signs()
    tables = density, lame, shear
    per = LANES // EDGE
    paired = {}

    for f in range(2):
        for c in range(3):
            for r in range(rows):
                x = vel_in[f * 3 + c, r]
                if f == 1 or c == 2:
                    x = x + first[f * (1 + c), V_ROWS + r]
                vel[f * 3 + c, r] = x
    for k, (f, c, d) in enumerate(FAR):
        for main, i, sign in zip(
            north_south(far_a, far_b, k), (S_ROWS - d, S_ROWS - 1 + d), signs
        ):
            halo[f * 6 + c - 3, i] = main * sign if FIELD_SIGNS[c] < 0 else main
    for f, c, d in NEAR:
        k = f * 6 + c - 3
        halo[k, S_ROWS - d] = stress[k, S_ROWS - d, :, :cols]
        halo[k, S_ROWS - 1 + d] = stress[k, S_ROWS + rows - 1 + d, :, :cols]

    def material(i, x, at):
        for n, value in enumerate(materials(x, dt, tables)):
            mats[n, i, :, at] = value

    main, side = slice(0, cols), slice(cols, cols + LANES)
    for r in range(rows):
        material(r + S_ROWS, strided(ids, r, levels, rows).astype(F32), main)
        v, slot = divmod(18 * rows + r, per)
        if v not in paired:
            paired[v] = paired_edges(id_edge_a, id_edge_b, v)
        material(r + S_ROWS, side_vector(paired[v], slot), side)
    for d in range(1, S_ROWS + 1):
        north, south = north_south(far_a, far_b, FAR_IDS + d - 1)
        material(S_ROWS - d, north, main)
        material(S_ROWS + rows - 1 + d, south, main)

    vectors = level_vectors(levels, width, dr, theta_step)

    def inner_first(r, carry):
        i = r + S_ROWS
        row_ap, row_cv = widened(ap[i], width), widened(cv[i], width)
        for f in range(2):
            new = stress_steps(vel, f, r, vectors, row_ap, row_cv, mats[1, i], mats[2, i], width)
            for n in range(6):
                inner_stress[f * 6 + n, r - INNER] = stress[f * 6 + n, i] + new[n]
        return carry

    lax.fori_loop(INNER, rows - INNER, inner_first, 0, unroll=4)

    def inner_second(r, carry):
        i = r + S_ROWS
        at = r - INNER - 2
        row_ap, row_cv = widened(ap[i], width), widened(cv[i], width)
        products = [vel[c, r, :, :cols] * vel[3 + c, r, :, :cols] for c in range(3)]
        fresh = []
        for f in range(2):
            steps = forces(inner_stress, f, r - INNER, vectors, row_ap, row_cv)
            for c, force in enumerate(steps):
                new = vel[f * 3 + c, r] + mats[0, i] * force
                if f == 1 or c == 2:
                    new = new + second[f * (1 + c), V_ROWS + r]
                inner_vel[f * 3 + c, at] = new
                fresh.append(new[:, :cols])
        products += [fresh[c] * fresh[3 + c] for c in range(3)]
        inner_density[at] = sum(products[1:], products[0])
        return carry

    lax.fori_loop(INNER + 2, rows - INNER - 2, inner_second, 0, unroll=4)


def final_kernel(
    dims, consts, vel_in, stress_in, halo, got_a, got_b, mats_in, first, second, ap, cv,
    inner_stress, inner_vel, inner_density, density_t, lame_t, shear_t,
    fwd_out, adj_out, density_out, vel, stress, mats, fwd, adj, density, sems,
):
    levels, rows, cols = dims
    dr, theta_step, dt = consts
    width = cols + LANES
    signs = pole_signs()
    tiles = cols // LANES
    side_at = slice(cols, width)
    plan, _ = side_plan()
    lanes_shape = (levels, LANES)

    def sides(kind, f, c, d):
        if (kind, f, c, d) not in plan:
            return (jnp.zeros(lanes_shape, F32),) * 2
        v, lane, wide = plan[kind, f, c, d]
        got = north_south(got_a, got_b, len(VEL) * tiles + v)
        return tuple(rolled(x, -lane - wide // 2) for x in got)

    def put_velocity(f, c, d, at, values):
        for x, i, sign in zip(values, (V_ROWS - d, V_ROWS + rows - 1 + d), signs):
            if FIELD_SIGNS[c] < 0:
                x = x * sign
            if f == 1 or c == 2:
                x = x + first[f * (1 + c), i, :, at]
            vel[f * 3 + c, i, :, at] = x

    for k, (f, c, d) in enumerate(VEL):
        for t in range(tiles):
            at = slice(t * LANES, (t + 1) * LANES)
            north, south = north_south(got_a, got_b, k * tiles + t)
            put_velocity(f, c, d, at, (north, south))
        put_velocity(f, c, d, side_at, sides("v", f, c, d))
    for f, c, d in NEAR + FAR:
        n = f * 6 + c - 3
        for x, i, i_main, sign in zip(
            sides("s", f, c, d),
            (S_ROWS - d, S_ROWS + rows - 1 + d),
            (S_ROWS - d, S_ROWS - 1 + d),
            signs,
        ):
            stress[n, i, :, side_at] = x * sign if FIELD_SIGNS[c] < 0 else x
            stress[n, i, :, :cols] = halo[n, i_main]
    for d in range(1, S_ROWS + 1):
        for x, i in zip(sides("i", 0, 0, d), (S_ROWS - d, S_ROWS + rows - 1 + d)):
            for n, value in enumerate(materials(x, dt, (density_t, lame_t, shear_t))):
                mats[n, i, :, side_at] = value
                mats[n, i, :, :cols] = mats_in[n, i, :, :cols]
    for n in range(3):
        for r in range(rows):
            mats[n, S_ROWS + r] = mats_in[n, S_ROWS + r]
    for k in range(6):
        for r in range(rows):
            vel[k, V_ROWS + r] = vel_in[k, r]
    for n in range(12):
        for r in range(INNER, rows - INNER):
            stress[n, S_ROWS + r] = inner_stress[n, r - INNER]

    vectors = level_vectors(levels, width, dr, theta_step)
    c1, c2 = vectors[1][:, :LANES], vectors[2][:, :LANES]

    def add_side(k, r, value):
        scale = mats[0, S_ROWS + r, :, side_at]
        vel[k, V_ROWS + r, :, side_at] = vel[k, V_ROWS + r, :, side_at] + scale * value

    for f in range(2):
        for c in range(3):
            k, n = f * 3 + c, f * 6 + CROSS[c] - 3
            n1, n2 = (stress[n, S_ROWS - d, :, side_at] for d in (1, 2))
            s1, s2 = (stress[n, S_ROWS + rows - 1 + d, :, side_at] for d in (1, 2))
            o1, o2 = (stress_in[n, S_ROWS + d, :, side_at] for d in (0, 1))
            u1, u2 = (stress_in[n, S_ROWS + rows - d, :, side_at] for d in (1, 2))
            add_side(k, 0, c2 * n2 - c1 * n1)
            add_side(k, 1, c2 * n1)
            add_side(k, rows - 1, c1 * s1 - c2 * s2)
            add_side(k, rows - 2, -(c2 * s1))
            add_side(k, -1, c1 * o1 - c2 * o2)
            add_side(k, -2, -(c2 * o1))
            add_side(k, rows, c2 * u2 - c1 * u1)
            add_side(k, rows + 1, c2 * u1)

    def first_stress(before, i, carry):
        row_ap, row_cv = widened(ap[i], width), widened(cv[i], width)
        lam, mu2 = mats[1, i], mats[2, i]
        for f in range(2):
            new = stress_steps(
                vel, f, i + V_ROWS - S_ROWS, vectors, row_ap, row_cv, lam, mu2, width
            )
            for n in range(6):
                stress[f * 6 + n, i] = before[f * 6 + n, i] + new[n]
        return carry

    inner = S_ROWS + rows
    lax.fori_loop(0, S_ROWS, functools.partial(first_stress, stress), 0, unroll=4)
    outer = functools.partial(first_stress, stress_in)
    lax.fori_loop(S_ROWS, S_ROWS + INNER, outer, 0, unroll=4)
    lax.fori_loop(inner - INNER, inner, outer, 0, unroll=4)
    lax.fori_loop(inner, inner + S_ROWS, functools.partial(first_stress, stress), 0, unroll=4)

    def second_velocity(own, r, carry):
        i = r + S_ROWS - 2
        j = r + V_ROWS - 2
        row_ap, row_cv = widened(ap[i], width), widened(cv[i], width)
        scale = mats[0, i]
        fresh, products = [], []
        if own:
            for c in range(3):
                products.append(vel[c, j, :, :cols] * vel[3 + c, j, :, :cols])
        for f in range(2):
            for c, force in enumerate(forces(stress, f, i, vectors, row_ap, row_cv)):
                new = vel[f * 3 + c, j] + scale * force
                if f == 1 or c == 2:
                    new = new + second[f * (1 + c), j]
                vel[f * 3 + c, j] = new
                fresh.append(new[:, :cols])
        if own:
            for c in range(3):
                products.append(fresh[c] * fresh[3 + c])
            density[pl.ds(r - 2, levels, stride=rows), :] = sum(products[1:], products[0])
            for f in range(2):
                for c in range(3):
                    at = c * levels * rows + r - 2
                    (fwd, adj)[f][pl.ds(at, levels, stride=rows), :] = fresh[f * 3 + c]
        return carry

    reach = INNER + 2
    own = functools.partial(second_velocity, True)
    lax.fori_loop(0, 2, functools.partial(second_velocity, False), 0, unroll=2)
    lax.fori_loop(2, 2 + reach, own, 0, unroll=6)
    lax.fori_loop(2 + rows - reach, 2 + rows, own, 0, unroll=6)
    lax.fori_loop(rows + 2, rows + 4, functools.partial(second_velocity, False), 0, unroll=2)
    for r in range(reach, rows - reach):
        density[pl.ds(r, levels, stride=rows), :] = inner_density[r - reach]
        for k in range(6):
            x = inner_vel[k, r - reach]
            vel[k, V_ROWS + r] = x
            at = k % 3 * levels * rows + r
            (fwd, adj)[k // 3][pl.ds(at, levels, stride=rows), :] = x[:, :cols]

    split = 3 * levels * rows
    early, late = pl.ds(0, split), pl.ds(split, 6 * levels * rows)
    copies = [
        pltpu.make_async_copy(fwd.at[early], fwd_out.at[early], sems.at[0]),
        pltpu.make_async_copy(adj.at[early], adj_out.at[early], sems.at[1]),
        pltpu.make_async_copy(density, density_out, sems.at[2]),
    ]
    for copy in copies:
        copy.start()

    def second_stress(r, carry):
        i = r + S_ROWS
        row_ap, row_cv = widened(ap[i], cols), widened(cv[i], cols)
        lam, mu2 = mats[1, i, :, :cols], mats[2, i, :, :cols]
        for f in range(2):
            new = stress_steps(vel, f, r + V_ROWS, vectors, row_ap, row_cv, lam, mu2, cols)
            for n in range(6):
                at = (3 + n) * levels * rows + r
                (fwd, adj)[f][pl.ds(at, levels, stride=rows), :] = (
                    stress[f * 6 + n, i, :, :cols] + new[n]
                )
        return carry

    lax.fori_loop(0, rows, second_stress, 0, unroll=8)
    copies += [
        pltpu.make_async_copy(fwd.at[late], fwd_out.at[late], sems.at[3]),
        pltpu.make_async_copy(adj.at[late], adj_out.at[late], sems.at[4]),
    ]
    for copy in copies[3:]:
        copy.start()
    for copy in copies:
        copy.wait()


def swap_tiles(x, first):
    count = lax.axis_size("lon")
    to = {i: (i + (1 if (i % 2 == 0) == first else -1)) % count for i in range(count)}
    return lax.ppermute(x, "lon", list(to.items()))


def swap_bands(x, first):
    bands, count = lax.axis_size("colat"), lax.axis_size("lon")
    pairs = []
    for lon in range(count):
        for band in range(bands):
            to_band, to_lon = band + (1 if (band % 2 == 0) == first else -1), lon
            if to_band < 0 or to_band >= bands:
                to_band, to_lon = band, (lon + count // 2) % count
            pairs.append((lon * bands + band, to_lon * bands + to_band))
    return lax.ppermute(x, ("lon", "colat"), pairs)


def call(kernel, out_shapes, specs, cost=0, out=None, **more):
    return pl.pallas_call(
        kernel,
        out_shape=out_shapes,
        in_specs=specs,
        out_specs=jax.tree.map(lambda _: out or vmem(), out_shapes),
        cost_estimate=pl.CostEstimate(flops=cost, bytes_accessed=cost, transcendentals=0),
        compiler_params=pltpu.CompilerParams(vmem_limit_bytes=16 * 2**20),
        **more,
    )


def on_device(
    forward_state, adjoint_state, layer_ids, density_table, lame_table, shear_table,
    source_cells, source_wavelet, receiver_cells, receiver_residual,
):
    dims = levels, rows, cols = layer_ids.shape
    lat_cells = rows * lax.axis_size("colat")
    lon_cells = cols * lax.axis_size("lon")
    dt = COURANT * SIN_FLOOR * R_INNER * (2.0 * math.pi / lon_cells) / 1.6
    consts = ((1.0 - R_INNER) / levels, math.pi / lat_cells, dt)
    width = cols + LANES
    tiles = cols // LANES

    def shape(*dims):
        return jax.ShapeDtypeStruct(dims, F32)

    parts = forward_state, adjoint_state
    state = jnp.concatenate([x.reshape(-1, rows, cols) for x in parts]).reshape(-1, cols)
    ids = layer_ids.reshape(levels * rows, cols)

    edges = shape(pieces(19 * rows, EDGE), levels, LANES)
    near = shape(len(NEAR), levels, cols)
    far = shape(len(FAR) + S_ROWS, levels, cols)
    extents = lat_cells, lon_cells
    edge_a, edge_b, near_a, near_b, far_a, far_b = call(
        functools.partial(pack_kernel, dims),
        [edges, edges, near, near, far, far],
        [vmem()] * 2,
        cost=10**6,
    )(state, ids)
    near_b = swap_bands(near_b, False)
    near_a = swap_bands(near_a, True)
    edge_b = swap_tiles(edge_b, False)
    edge_a = swap_tiles(edge_a, True)
    far_b = swap_bands(far_b, False)
    far_a = swap_bands(far_a, True)

    ap, cv = geometry(dims, extents)
    count = max(LANES, receiver_cells.shape[0])

    def lines(x):
        x = x.astype(F32).reshape(-1, x.shape[-1])
        return jnp.pad(x, ((0, 0), (0, count - x.shape[1])))

    given = jnp.concatenate(
        [lines(x) for x in (receiver_cells, receiver_residual, source_cells, source_wavelet)]
    )
    leaving = shape(len(VEL) * tiles + side_plan()[1], levels, LANES)
    stress_shape = shape(12, rows + 2 * S_ROWS, levels, width)
    mats_shape = shape(3, rows + 2 * S_ROWS, levels, width)
    vel_shape = shape(6, rows, levels, width)
    stress, vel, rho, id_side, pay_b = call(
        functools.partial(velocity_kernel, dims, consts),
        [stress_shape, vel_shape, shape(rows, levels, width), shape(rows, levels, LANES), leaving],
        [vmem()] * 9 + [smem()],
        cost=10**7,
    )(state, ids, edge_a, edge_b, near_a, near_b, ap, cv, given, density_table)
    got_b = swap_bands(pay_b, False)
    vel, pay_a = call(
        functools.partial(rest_kernel, dims, consts), [vel_shape, leaving], [vmem()] * 6, cost=10**7
    )(stress, vel, rho, id_side, ap, cv)
    got_a = swap_bands(pay_a, True)

    first, second = call(
        functools.partial(inject_kernel, dims, extents),
        [shape(4, rows + 2 * V_ROWS, levels, width)] * 2,
        [vmem()],
        cost=10**8,
    )(given)
    halo, mats, full_vel, inner_stress, inner_vel, inner_density = call(
        functools.partial(fill_kernel, dims, consts),
        [
            shape(12, 2 * S_ROWS, levels, cols),
            mats_shape,
            vel_shape,
            shape(12, rows - 2 * INNER, levels, width),
            shape(6, rows - 2 * INNER - 4, levels, width),
            shape(rows - 2 * INNER - 4, levels, cols),
        ],
        [vmem()] * 11 + [smem()] * 3,
        cost=10**8,
    )(
        stress, vel, ids, edge_a, edge_b, far_a, far_b, first, second, ap, cv,
        density_table, lame_table, shear_table,
    )

    flat = (9 * levels * rows, cols), (9 * levels * rows, cols), (levels * rows, cols)
    fwd, adj, density = call(
        functools.partial(final_kernel, dims, consts),
        [shape(*x) for x in flat],
        [vmem()] * 13 + [smem()] * 3,
        cost=10**8,
        out=pl.BlockSpec(memory_space=pltpu.HBM),
        scratch_shapes=[
            pltpu.VMEM((6, rows + 2 * V_ROWS, levels, width), F32),
            pltpu.VMEM(stress_shape.shape, F32),
            pltpu.VMEM(mats_shape.shape, F32),
        ]
        + [pltpu.VMEM(x, F32) for x in flat]
        + [pltpu.SemaphoreType.DMA((5,))],
    )(
        full_vel, stress, halo, got_a, got_b, mats, first, second, ap, cv,
        inner_stress, inner_vel, inner_density, density_table, lame_table, shear_table,
    )
    return (
        fwd.reshape(forward_state.shape),
        adj.reshape(adjoint_state.shape),
        density.reshape(layer_ids.shape),
    )


def solution(mesh):
    return jax.shard_map(
        on_device,
        mesh=mesh,
        in_specs=(
            P(None, None, "colat", "lon"),
            P(None, None, "colat", "lon"),
            P(None, "colat", "lon"),
        )
        + (P(),) * 7,
        out_specs=(
            P(None, None, "colat", "lon"),
            P(None, None, "colat", "lon"),
            P(None, "colat", "lon"),
        ),
        check_vma=False,
    )
```

```python
import functools
import math

import jax
import jax.numpy as jnp
from jax import lax
from jax.experimental import pallas as pl
from jax.experimental.pallas import tpu as pltpu
from jax.sharding import PartitionSpec as P

R_INNER = 0.55
COURANT = 0.3
SIN_FLOOR = 0.25
FIELD_SIGNS = (-1, -1, 1, 1, 1, 1, 1, -1, -1)
CROSS = (3, 6, 7)
OTHER = (4, 5, 8)
EDGE = 8
LANES = 128
V_ROWS = 6
S_ROWS = 4
INNER = 2
F32 = jnp.float32


NEAR = tuple((f, c, d) for f in range(2) for c in CROSS for d in (1, 2))
FAR = tuple((f, c, d) for f in range(2) for c in OTHER for d in (1, 2)) + tuple(
    (f, c, d) for f in range(2) for c in CROSS for d in (3, 4)
)
FAR_IDS = len(FAR)
VEL = tuple((f, c, d) for f in range(2) for c in range(3) for d in range(1, V_ROWS + 1))


def vmem():
    return pl.BlockSpec(memory_space=pltpu.VMEM)


def smem():
    return pl.BlockSpec(memory_space=pltpu.SMEM)


def lane_iota(shape):
    return lax.broadcasted_iota(jnp.int32, shape, 1)


def rolled(x, shift, axis=1):
    size = x.shape[axis]
    shift = shift % size
    return x if shift == 0 else pltpu.roll(x, shift, axis)


def side_plan():
    wide = [("v", f, c, 1) for f in range(2) for c in range(3)]
    wide += [("s",) + entry for entry in NEAR] + [("i", 0, 0, 1)]
    slim = [("v", f, c, d) for f, c, d in VEL if 1 < d < V_ROWS]
    slim += [("s",) + entry for entry in FAR if entry[2] < S_ROWS] + [("i", 0, 0, 2), ("i", 0, 0, 3)]
    plan, lane = {}, 0
    for width, entries in ((2 * EDGE, wide), (EDGE, slim)):
        for entry in entries:
            plan[entry] = (lane // LANES, lane % LANES, width)
            lane += width
    return plan, -(-lane // LANES)


def pieces(count, width):
    per = LANES // width
    return -(-count // per)


def paired_edges(edge_a, edge_b, v):
    a, b = edge_a[v], edge_b[v]
    even = even_tile()
    after, before = jnp.where(even, a, b), jnp.where(even, b, a)
    odd_lane = lax.rem(lane_iota(a.shape) // EDGE, 2) == 1
    return jnp.where(odd_lane, before, after), jnp.where(odd_lane, after, before)


def side_vector(paired, slot):
    return rolled(paired[slot % 2], -slot * EDGE)


def even_band():
    return lax.rem(lax.axis_index("colat"), 2) == 0


def even_tile():
    return lax.rem(lax.axis_index("lon"), 2) == 0


def pole_signs():
    band, last = lax.axis_index("colat"), lax.axis_size("colat") - 1
    north = jnp.where(band == 0, -1.0, 1.0).astype(F32)
    south = jnp.where(band == last, -1.0, 1.0).astype(F32)
    return north, south


def strided(ref, first, levels, rows):
    return ref[pl.ds(first, levels, stride=rows), :]


def pack_kernel(dims, state, ids, edge_a, edge_b, near_a, near_b, far_a, far_b):
    levels, rows, cols = dims
    even = even_band()

    def row(f, c, r):
        return strided(state, (f * 9 + c) * levels * rows + r, levels, rows)

    def id_row(r):
        return strided(ids, r, levels, rows).astype(F32)

    def put(ref_a, ref_b, k, get, d):
        top, bottom = get(d - 1), get(rows - d)
        ref_a[k], ref_b[k] = jnp.where(even, bottom, top), jnp.where(even, top, bottom)

    for k, (f, c, d) in enumerate(NEAR):
        put(near_a, near_b, k, functools.partial(row, f, c), d)
    for k, (f, c, d) in enumerate(FAR):
        put(far_a, far_b, k, functools.partial(row, f, c), d)
    for d in range(1, S_ROWS + 1):
        put(far_a, far_b, FAR_IDS + d - 1, id_row, d)

    per = LANES // EDGE
    edges = [functools.partial(row, f, c, r) for f in range(2) for c in range(9) for r in range(rows)]
    edges += [functools.partial(id_row, r) for r in range(rows)]
    lane = lane_iota((levels, LANES))
    swapped = jnp.logical_not(even_tile())
    for v in range(edge_a.shape[0]):
        east = west = None
        for slot, get in reversed(list(enumerate(edges[v * per : (v + 1) * per]))):
            x = get()
            last = rolled(x[:, cols - LANES :], slot * EDGE)
            first = last if cols == LANES else rolled(x[:, :LANES], slot * EDGE)
            if east is None:
                east, west = last, first
            else:
                west = jnp.where(lane < (slot + 1) * EDGE, first, west)
                if slot:
                    east = jnp.where(lane < slot * EDGE, last, east)
                else:
                    east = jnp.where(lane < LANES - EDGE, east, last)
        edge_a[v] = jnp.where(swapped, west, east)
        edge_b[v] = jnp.where(swapped, east, west)


def divided(x, by):
    q = jnp.floor(x.astype(F32) * (1.0 / by)).astype(jnp.int32)
    r = x - q * by
    q = q + jnp.where(r >= by, 1, 0) - jnp.where(r < 0, 1, 0)
    return q, x - q * by


def inject_kernel(dims, extents, given, first, second):
    levels, rows, cols = dims
    lat_cells, lon_cells = extents
    width = cols + LANES
    signs = (1.0,) + pole_signs()
    first_row, first_col = lax.axis_index("colat") * rows, lax.axis_index("lon") * cols
    at_top, at_bottom = first_row == 0, first_row + rows == lat_cells
    half = lon_cells // 2

    def located(ids):
        level, rest = divided(ids, lat_cells * lon_cells)
        row, col = divided(rest, lon_cells)

        def lane(c):
            x = c - first_col
            x = jnp.where(x < 0, x + lon_cells, x)
            x = jnp.where(x >= lon_cells, x - lon_cells, x)
            tail = x - lon_cells + cols + LANES
            tail = jnp.where(tail >= cols + LANES - EDGE, tail, -1)
            return jnp.where(x < cols + EDGE, x, tail)

        def code(r, count):
            inside = jnp.logical_and(r >= 0, r < count)
            return jnp.where(inside, r * levels + level, -1)

        north = V_ROWS - 1 - jnp.where(at_top, row, first_row - 1 - row)
        south = jnp.where(at_bottom, lat_cells - 1 - row, row - first_row - rows)
        return (
            (code(row - first_row, rows), lane(col)),
            (code(north, V_ROWS), lane(jnp.where(at_top, col + half, col))),
            (code(south, V_ROWS), lane(jnp.where(at_bottom, col + half, col))),
        )

    def parts(value):
        out, rest = [], value
        for _ in range(3):
            part = rest.astype(jnp.bfloat16)
            out.append(part)
            rest = rest - part.astype(F32)
        return out

    def hot(ids, size):
        same = lax.broadcasted_iota(jnp.int32, (size, ids.shape[1]), 0) == ids
        return jnp.where(same, 1.0, 0.0).astype(jnp.bfloat16)

    def line(n, size):
        return given[n : n + 1, :size]

    places = located(line(0, None).astype(jnp.int32))
    splaces = located(line(7, LANES).astype(jnp.int32))
    regions = ((V_ROWS, rows), (0, V_ROWS), (V_ROWS + rows, V_ROWS))
    receivers = [(s, 1 + c, parts(line(1 + 3 * s + c, None))) for s in range(2) for c in range(3)]
    sources = [(s, 0, parts(line(8 + s, LANES))) for s in range(2)]
    for n, (at, count) in enumerate(regions):
        size = count * levels
        for place, todo in ((places[n], receivers), (splaces[n], sources)):
            on_row, on_lane = hot(place[0], size), hot(place[1], width)
            stacked = jnp.concatenate([on_row * part for _, _, three in todo for part in three])
            spread = lax.dot_general(
                stacked, on_lane, (((1,), (1,)), ((), ())), preferred_element_type=F32
            )
            for m, (s, k, _) in enumerate(todo):
                rest = [spread[(3 * m + p) * size : (3 * m + p + 1) * size] for p in range(3)]
                total = rest[0] + rest[1] + rest[2]
                if n and k and FIELD_SIGNS[k - 1] < 0:
                    total = total * signs[n]
                (first, second)[s][k, at : at + count] = total.reshape(count, levels, width)


def geometry(dims, extents):
    levels, rows, _ = dims
    lat_cells, lon_cells = extents
    first_row = lax.axis_index("colat") * rows
    g = first_row + jnp.arange(-S_ROWS, rows + S_ROWS, dtype=jnp.int32)
    sign = jnp.where(jnp.logical_or(g < 0, g >= lat_cells), -1.0, 1.0)
    g = jnp.where(g < 0, -1 - g, jnp.where(g >= lat_cells, 2 * lat_cells - 1 - g, g))
    angle = (g.astype(F32) + 0.5) * (math.pi / lat_cells)
    held = jnp.maximum(jnp.sin(angle), SIN_FLOOR)
    pair = sign / (held * (24.0 * math.pi / lon_cells)), sign * jnp.cos(angle) / held
    pair = lax.optimization_barrier(pair)
    k = jnp.arange(levels, dtype=F32)
    ir = 1.0 / (R_INNER + (k + 0.5) * ((1.0 - R_INNER) / levels))
    shape = g.shape[0], levels, LANES
    return tuple(
        jnp.broadcast_to(x[:, None, None] * ir[None, :, None], shape) for x in pair
    )


def level_vectors(levels, width, dr, theta_step):
    k = lax.broadcasted_iota(jnp.int32, (levels, width), 0)
    ir = 1.0 / (R_INNER + (k.astype(F32) + 0.5) * dr)
    up = jnp.where(k < levels - 1, 0.5 / dr, 0.0).astype(F32)
    down = jnp.where(k > 0, 0.5 / dr, 0.0).astype(F32)
    return ir, ir * (8.0 / 12.0 / theta_step), ir * (1.0 / 12.0 / theta_step), up, down


def along_theta(ref, k, i, c1, c2):
    return c1 * (ref[k, i + 1] - ref[k, i - 1]) - c2 * (ref[k, i + 2] - ref[k, i - 2])


def along_phi(x):
    return 8.0 * (rolled(x, -1) - rolled(x, 1)) - (rolled(x, -2) - rolled(x, 2))


def along_r(x, up, down):
    return up * rolled(x, -1, 0) - down * rolled(x, 1, 0)


def forces(stress, f, i, vectors, ap, cv):
    ir, c1, c2, up, down = vectors
    k = f * 6
    tt, pp, rr, tp, tr, pr = (stress[k + n, i] for n in range(6))
    f_t = (
        along_theta(stress, k, i, c1, c2)
        + ap * along_phi(tp)
        + along_r(tr, up, down)
        + cv * (tt - pp)
        + 3.0 * (ir * tr)
    )
    f_p = (
        along_theta(stress, k + 3, i, c1, c2)
        + ap * along_phi(pp)
        + along_r(pr, up, down)
        + 2.0 * (cv * tp)
        + 3.0 * (ir * pr)
    )
    f_r = (
        along_theta(stress, k + 4, i, c1, c2)
        + ap * along_phi(pr)
        + along_r(rr, up, down)
        + ir * (2.0 * rr - tt - pp)
        + cv * tr
    )
    return f_t, f_p, f_r


def stress_steps(vel, f, i, vectors, ap, cv, lam, mu2, keep):
    ir, c1, c2, up, down = (v[:, :keep] for v in vectors)
    k = f * 3
    whole = tuple(vel[k + n, i] for n in range(3))
    v_t, v_p, v_r = (x[:, :keep] for x in whole)
    p_t, p_p, p_r = (along_phi(x)[:, :keep] for x in whole)

    def theta(n):
        return c1 * (vel[k + n, i + 1, :, :keep] - vel[k + n, i - 1, :, :keep]) - c2 * (
            vel[k + n, i + 2, :, :keep] - vel[k + n, i - 2, :, :keep]
        )

    ir_r = ir * v_r
    e_tt = theta(0) + ir_r
    e_pp = ap * p_p + cv * v_t + ir_r
    e_rr = along_r(v_r, up, down)
    e_tp = theta(1) - cv * v_p + ap * p_t
    e_tr = along_r(v_t, up, down) - ir * v_t + theta(2)
    e_pr = along_r(v_p, up, down) - ir * v_p + ap * p_r
    bulk = lam * (e_tt + e_pp + e_rr)
    half_mu = 0.5 * mu2
    return (
        bulk + mu2 * e_tt,
        bulk + mu2 * e_pp,
        bulk + mu2 * e_rr,
        half_mu * e_tp,
        half_mu * e_tr,
        half_mu * e_pr,
    )


def look_up(ids, tables):
    out = [jnp.full(ids.shape, table[0], F32) for table in tables]
    for n in range(1, tables[0].shape[0]):
        hit = ids == float(n)
        out = [jnp.where(hit, table[n], x) for table, x in zip(tables, out)]
    return out


def materials(ids, dt, tables):
    rho, lam, mu = look_up(ids, tables)
    return dt / rho, dt * lam, (2.0 * dt) * mu


def widened(x, width):
    return jnp.concatenate([x] * (width // LANES), axis=1)


def north_south(ref_a, ref_b, k):
    even = even_band()
    a, b = ref_a[k], ref_b[k]
    return jnp.where(even, b, a), jnp.where(even, a, b)


def velocity_kernel(
    dims, consts, state, ids, edge_a, edge_b, near_a, near_b, ap, cv, given, density,
    stress, vel, rho, id_side, pay_b,
):
    levels, rows, cols = dims
    _, _, dt = consts
    signs = pole_signs()
    per = LANES // EDGE
    paired = {}

    def side_of(j):
        if j // per not in paired:
            paired[j // per] = paired_edges(edge_a, edge_b, j // per)
        return side_vector(paired[j // per], j % per)

    for f in range(2):
        for c in range(9):
            for r in range(rows):
                main = strided(state, (f * 9 + c) * levels * rows + r, levels, rows)
                side = side_of((f * 9 + c) * rows + r)
                if c < 3:
                    ref, k, i = vel, f * 3 + c, r
                else:
                    ref, k, i = stress, f * 6 + c - 3, r + S_ROWS
                ref[k, i, :, :cols] = main
                ref[k, i, :, cols:] = side
    for r in range(rows):
        main = strided(ids, r, levels, rows).astype(F32)
        side = side_of(18 * rows + r)
        id_side[r] = side
        rho[r, :, :cols] = dt / look_up(main, (density,))[0]
        rho[r, :, cols:] = dt / look_up(side, (density,))[0]
    for k, (f, c, d) in enumerate(NEAR):
        for main, i, sign in zip(
            north_south(near_a, near_b, k), (S_ROWS - d, S_ROWS + rows - 1 + d), signs
        ):
            if FIELD_SIGNS[c] < 0:
                main = main * sign
            stress[f * 6 + c - 3, i, :, :cols] = main
            stress[f * 6 + c - 3, i, :, cols:] = jnp.zeros((levels, LANES), F32)

    base = jnp.where(even_band(), 0, rows - V_ROWS)
    step = velocity_step(dims, consts, stress, vel, vel, rho, ap, cv)
    lax.fori_loop(0, V_ROWS, lambda q, carry: step(base + q, carry), 0, unroll=V_ROWS)
    payload(dims, jnp.logical_not(even_band()), stress, vel, id_side, pay_b)


def rest_kernel(dims, consts, stress, vel_in, rho, id_side, ap, cv, vel, pay_a):
    _, rows, _ = dims
    done = jnp.where(even_band(), 0, rows - V_ROWS)
    base = jnp.where(even_band(), V_ROWS, 0)
    for q in range(V_ROWS):
        for k in range(6):
            vel[k, done + q] = vel_in[k, done + q]
    step = velocity_step(dims, consts, stress, vel_in, vel, rho, ap, cv)
    lax.fori_loop(0, rows - V_ROWS, lambda q, carry: step(base + q, carry), 0, unroll=5)
    payload(dims, even_band(), stress, vel, id_side, pay_a)


def velocity_step(dims, consts, stress, before, after, rho, ap, cv):
    levels, _, cols = dims
    dr, theta_step, _ = consts
    width = cols + LANES
    vectors = level_vectors(levels, width, dr, theta_step)

    def step(r, carry):
        i = r + S_ROWS
        scale = rho[r]
        row_ap, row_cv = widened(ap[i], width), widened(cv[i], width)
        for f in range(2):
            for c, force in enumerate(forces(stress, f, i, vectors, row_ap, row_cv)):
                after[f * 3 + c, r] = before[f * 3 + c, r] + scale * force
        return carry

    return step


def payload(dims, bottom_side, stress, vel, id_side, ref):
    levels, rows, cols = dims
    tiles = cols // LANES
    plan, vectors_out = side_plan()

    def facing(d):
        return jnp.where(bottom_side, rows - d, d - 1)

    for k, (f, c, d) in enumerate(VEL):
        for t in range(tiles):
            at = slice(t * LANES, (t + 1) * LANES)
            ref[k * tiles + t] = vel[f * 3 + c, facing(d), :, at]
    packed, lanes = [None] * vectors_out, lane_iota((levels, LANES))
    for (kind, f, c, d), (v, lane, wide) in plan.items():
        if kind == "v":
            x = vel[f * 3 + c, facing(d), :, cols:]
        elif kind == "s":
            x = stress[f * 6 + c - 3, facing(d) + S_ROWS, :, cols:]
        else:
            x = id_side[facing(d)]
        x = rolled(x, lane + wide // 2)
        packed[v] = x if packed[v] is None else jnp.where(lanes >= lane, x, packed[v])
    for v, x in enumerate(packed):
        ref[len(VEL) * tiles + v] = x


def fill_kernel(
    dims, consts, stress, vel_in, ids, id_edge_a, id_edge_b, far_a, far_b, first, second, ap, cv,
    density, lame, shear, halo, mats, vel, inner_stress, inner_vel, inner_density, inner_last,
):
    levels, rows, cols = dims
    dr, theta_step, dt = consts
    width = cols + LANES
    signs = pole_signs()
    tables = density, lame, shear
    per = LANES // EDGE
    paired = {}

    for f in range(2):
        for c in range(3):
            for r in range(rows):
                x = vel_in[f * 3 + c, r]
                if f == 1 or c == 2:
                    x = x + first[f * (1 + c), V_ROWS + r]
                vel[f * 3 + c, r] = x
    for k, (f, c, d) in enumerate(FAR):
        for main, i, sign in zip(
            north_south(far_a, far_b, k), (S_ROWS - d, S_ROWS - 1 + d), signs
        ):
            halo[f * 6 + c - 3, i] = main * sign if FIELD_SIGNS[c] < 0 else main
    for f, c, d in NEAR:
        k = f * 6 + c - 3
        halo[k, S_ROWS - d] = stress[k, S_ROWS - d, :, :cols]
        halo[k, S_ROWS - 1 + d] = stress[k, S_ROWS + rows - 1 + d, :, :cols]

    def material(i, x, at):
        for n, value in enumerate(materials(x, dt, tables)):
            mats[n, i, :, at] = value

    main, side = slice(0, cols), slice(cols, cols + LANES)
    for r in range(rows):
        material(r + S_ROWS, strided(ids, r, levels, rows).astype(F32), main)
        v, slot = divmod(18 * rows + r, per)
        if v not in paired:
            paired[v] = paired_edges(id_edge_a, id_edge_b, v)
        material(r + S_ROWS, side_vector(paired[v], slot), side)
    for d in range(1, S_ROWS + 1):
        north, south = north_south(far_a, far_b, FAR_IDS + d - 1)
        material(S_ROWS - d, north, main)
        material(S_ROWS + rows - 1 + d, south, main)

    vectors = level_vectors(levels, width, dr, theta_step)

    def inner_first(r, carry):
        i = r + S_ROWS
        row_ap, row_cv = widened(ap[i], width), widened(cv[i], width)
        for f in range(2):
            new = stress_steps(vel, f, r, vectors, row_ap, row_cv, mats[1, i], mats[2, i], width)
            for n in range(6):
                inner_stress[f * 6 + n, r - INNER] = stress[f * 6 + n, i] + new[n]
        return carry

    lax.fori_loop(INNER, rows - INNER, inner_first, 0, unroll=4)

    def inner_second(r, carry):
        i = r + S_ROWS
        at = r - INNER - 2
        row_ap, row_cv = widened(ap[i], width), widened(cv[i], width)
        products = [vel[c, r, :, :cols] * vel[3 + c, r, :, :cols] for c in range(3)]
        fresh = []
        for f in range(2):
            steps = forces(inner_stress, f, r - INNER, vectors, row_ap, row_cv)
            for c, force in enumerate(steps):
                new = vel[f * 3 + c, r] + mats[0, i] * force
                if f == 1 or c == 2:
                    new = new + second[f * (1 + c), V_ROWS + r]
                inner_vel[f * 3 + c, at] = new
                fresh.append(new[:, :cols])
        products += [fresh[c] * fresh[3 + c] for c in range(3)]
        inner_density[at] = sum(products[1:], products[0])
        return carry

    lax.fori_loop(INNER + 2, rows - INNER - 2, inner_second, 0, unroll=4)

    def inner_third(r, carry):
        i = r + S_ROWS
        row_ap, row_cv = widened(ap[i], cols), widened(cv[i], cols)
        lam, mu2 = mats[1, i, :, :cols], mats[2, i, :, :cols]
        for f in range(2):
            new = stress_steps(
                inner_vel, f, r - INNER - 2, vectors, row_ap, row_cv, lam, mu2, cols
            )
            for n in range(6):
                old = inner_stress[f * 6 + n, r - INNER, :, :cols]
                inner_last[f * 6 + n, r - INNER - 4] = old + new[n]
        return carry

    lax.fori_loop(INNER + 4, rows - INNER - 4, inner_third, 0, unroll=4)


def final_kernel(
    dims, consts, vel_in, stress_in, halo, got_a, got_b, mats_in, first, second, ap, cv,
    inner_stress, inner_vel, inner_density, inner_last, density_t, lame_t, shear_t,
    fwd_out, adj_out, density_out, vel, stress, mats, fwd, adj, density, sems,
):
    levels, rows, cols = dims
    dr, theta_step, dt = consts
    width = cols + LANES
    signs = pole_signs()
    tiles = cols // LANES
    side_at = slice(cols, width)
    plan, _ = side_plan()
    lanes_shape = (levels, LANES)

    def sides(kind, f, c, d):
        if (kind, f, c, d) not in plan:
            return (jnp.zeros(lanes_shape, F32),) * 2
        v, lane, wide = plan[kind, f, c, d]
        got = north_south(got_a, got_b, len(VEL) * tiles + v)
        return tuple(rolled(x, -lane - wide // 2) for x in got)

    def put_velocity(f, c, d, at, values):
        for x, i, sign in zip(values, (V_ROWS - d, V_ROWS + rows - 1 + d), signs):
            if FIELD_SIGNS[c] < 0:
                x = x * sign
            if f == 1 or c == 2:
                x = x + first[f * (1 + c), i, :, at]
            vel[f * 3 + c, i, :, at] = x

    for k, (f, c, d) in enumerate(VEL):
        for t in range(tiles):
            at = slice(t * LANES, (t + 1) * LANES)
            north, south = north_south(got_a, got_b, k * tiles + t)
            put_velocity(f, c, d, at, (north, south))
        put_velocity(f, c, d, side_at, sides("v", f, c, d))
    for f, c, d in NEAR + FAR:
        n = f * 6 + c - 3
        for x, i, i_main, sign in zip(
            sides("s", f, c, d),
            (S_ROWS - d, S_ROWS + rows - 1 + d),
            (S_ROWS - d, S_ROWS - 1 + d),
            signs,
        ):
            stress[n, i, :, side_at] = x * sign if FIELD_SIGNS[c] < 0 else x
            stress[n, i, :, :cols] = halo[n, i_main]
    for d in range(1, S_ROWS + 1):
        for x, i in zip(sides("i", 0, 0, d), (S_ROWS - d, S_ROWS + rows - 1 + d)):
            for n, value in enumerate(materials(x, dt, (density_t, lame_t, shear_t))):
                mats[n, i, :, side_at] = value
                mats[n, i, :, :cols] = mats_in[n, i, :, :cols]
    reach = INNER + 2
    last = INNER + 4
    border = [*range(last), *range(rows - last, rows)]
    for n in range(3):
        for r in border:
            mats[n, S_ROWS + r] = mats_in[n, S_ROWS + r]
    for k in range(6):
        for r in range(rows):
            if not reach <= r < rows - reach:
                vel[k, V_ROWS + r] = vel_in[k, r]
    for n in range(12):
        for r in border:
            if INNER <= r < rows - INNER:
                stress[n, S_ROWS + r] = inner_stress[n, r - INNER]

    vectors = level_vectors(levels, width, dr, theta_step)
    c1, c2 = vectors[1][:, :LANES], vectors[2][:, :LANES]

    def add_side(k, r, value):
        value = mats[0, S_ROWS + r, :, side_at] * value
        vel[k, V_ROWS + r, :, side_at] = vel[k, V_ROWS + r, :, side_at] + value
        return value

    def spread_theta(near_row, far_row, south):
        if south:
            return c1 * near_row - c2 * far_row, -(c2 * near_row)
        return c2 * far_row - c1 * near_row, c2 * near_row

    changes = []
    for f in range(2):
        for c in range(3):
            k, n = f * 3 + c, f * 6 + CROSS[c] - 3
            n1, n2 = (stress[n, S_ROWS - d, :, side_at] for d in (1, 2))
            s1, s2 = (stress[n, S_ROWS + rows - 1 + d, :, side_at] for d in (1, 2))
            o1, o2 = (stress_in[n, S_ROWS + d, :, side_at] for d in (0, 1))
            u1, u2 = (stress_in[n, S_ROWS + rows - d, :, side_at] for d in (1, 2))
            top = add_side(k, 0, c2 * n2 - c1 * n1), add_side(k, 1, c2 * n1)
            bottom = add_side(k, rows - 1, c1 * s1 - c2 * s2), add_side(k, rows - 2, -(c2 * s1))
            changes.append(
                (spread_theta(top[1], top[0], False), spread_theta(bottom[1], bottom[0], True))
            )
            add_side(k, -1, c1 * o1 - c2 * o2)
            add_side(k, -2, -(c2 * o1))
            add_side(k, rows, c2 * u2 - c1 * u1)
            add_side(k, rows + 1, c2 * u1)

    later = []
    for f in range(2):
        for south in range(2):
            steps = []
            for m in range(2):
                i = S_ROWS + (rows - 1 - INNER - m if south else INNER + m)
                d_t, d_p, d_r = (changes[f * 3 + c][south][m] for c in range(3))
                lam, mu2 = mats[1, i, :, side_at], mats[2, i, :, side_at]
                bulk, half_mu = lam * d_t, 0.5 * mu2
                added = bulk + mu2 * d_t, bulk, bulk, half_mu * d_p, half_mu * d_r
                for n, x in enumerate(added):
                    stress[f * 6 + n, i, :, side_at] = stress[f * 6 + n, i, :, side_at] + x
                steps.append((added[0], added[3], added[4]))
            for c in range(3):
                moved = spread_theta(steps[1][c], steps[0][c], south)
                for m in range(2):
                    r = rows - 1 - reach - m if south else reach + m
                    later.append((f * 3 + c, r, moved[m]))

    def first_stress(before, i, carry):
        row_ap, row_cv = widened(ap[i], width), widened(cv[i], width)
        lam, mu2 = mats[1, i], mats[2, i]
        for f in range(2):
            new = stress_steps(
                vel, f, i + V_ROWS - S_ROWS, vectors, row_ap, row_cv, lam, mu2, width
            )
            for n in range(6):
                stress[f * 6 + n, i] = before[f * 6 + n, i] + new[n]
        return carry

    inner = S_ROWS + rows
    lax.fori_loop(0, S_ROWS, functools.partial(first_stress, stress), 0, unroll=4)
    outer = functools.partial(first_stress, stress_in)
    lax.fori_loop(S_ROWS, S_ROWS + INNER, outer, 0, unroll=INNER)
    lax.fori_loop(inner - INNER, inner, outer, 0, unroll=INNER)
    lax.fori_loop(inner, inner + S_ROWS, functools.partial(first_stress, stress), 0, unroll=4)

    def second_velocity(own, r, carry):
        i = r + S_ROWS - 2
        j = r + V_ROWS - 2
        row_ap, row_cv = widened(ap[i], width), widened(cv[i], width)
        scale = mats[0, i]
        fresh, products = [], []
        if own:
            for c in range(3):
                products.append(vel[c, j, :, :cols] * vel[3 + c, j, :, :cols])
        for f in range(2):
            for c, force in enumerate(forces(stress, f, i, vectors, row_ap, row_cv)):
                new = vel[f * 3 + c, j] + scale * force
                if f == 1 or c == 2:
                    new = new + second[f * (1 + c), j]
                vel[f * 3 + c, j] = new
                fresh.append(new[:, :cols])
        if own:
            for c in range(3):
                products.append(fresh[c] * fresh[3 + c])
            density[pl.ds(r - 2, levels, stride=rows), :] = sum(products[1:], products[0])
            for f in range(2):
                for c in range(3):
                    at = c * levels * rows + r - 2
                    (fwd, adj)[f][pl.ds(at, levels, stride=rows), :] = fresh[f * 3 + c]
        return carry

    own = functools.partial(second_velocity, True)
    lax.fori_loop(0, 2, functools.partial(second_velocity, False), 0, unroll=2)
    lax.fori_loop(2, 2 + reach, own, 0, unroll=reach)
    lax.fori_loop(2 + rows - reach, 2 + rows, own, 0, unroll=reach)
    lax.fori_loop(rows + 2, rows + 4, functools.partial(second_velocity, False), 0, unroll=2)
    for r in range(reach, rows - reach):
        density[pl.ds(r, levels, stride=rows), :] = inner_density[r - reach]
        for k in range(6):
            x = inner_vel[k, r - reach]
            vel[k, V_ROWS + r] = x
            at = k % 3 * levels * rows + r
            (fwd, adj)[k // 3][pl.ds(at, levels, stride=rows), :] = x[:, :cols]
    for k, r, value in later:
        add_side(k, r, value)

    split = 3 * levels * rows
    early, late = pl.ds(0, split), pl.ds(split, 6 * levels * rows)
    copies = [
        pltpu.make_async_copy(fwd.at[early], fwd_out.at[early], sems.at[0]),
        pltpu.make_async_copy(adj.at[early], adj_out.at[early], sems.at[1]),
        pltpu.make_async_copy(density, density_out, sems.at[2]),
    ]
    for copy in copies:
        copy.start()

    def second_stress(f, r, carry):
        i = r + S_ROWS
        row_ap, row_cv = widened(ap[i], cols), widened(cv[i], cols)
        lam, mu2 = mats[1, i, :, :cols], mats[2, i, :, :cols]
        new = stress_steps(vel, f, r + V_ROWS, vectors, row_ap, row_cv, lam, mu2, cols)
        for n in range(6):
            at = (3 + n) * levels * rows + r
            (fwd, adj)[f][pl.ds(at, levels, stride=rows), :] = (
                stress[f * 6 + n, i, :, :cols] + new[n]
            )
        return carry

    for f, (x, x_out) in enumerate(((fwd, fwd_out), (adj, adj_out))):
        for n in range(6):
            for r in range(last, rows - last):
                at = (3 + n) * levels * rows + r
                x[pl.ds(at, levels, stride=rows), :] = inner_last[f * 6 + n, r - last]
        finish = functools.partial(second_stress, f)
        lax.fori_loop(0, last, finish, 0, unroll=last)
        lax.fori_loop(rows - last, rows, finish, 0, unroll=last)
        copies.append(pltpu.make_async_copy(x.at[late], x_out.at[late], sems.at[3 + f]))
        copies[-1].start()
    for copy in copies:
        copy.wait()


def swap_tiles(x, first):
    count = lax.axis_size("lon")
    to = {i: (i + (1 if (i % 2 == 0) == first else -1)) % count for i in range(count)}
    return lax.ppermute(x, "lon", list(to.items()))


def swap_bands(x, first):
    bands, count = lax.axis_size("colat"), lax.axis_size("lon")
    pairs = []
    for lon in range(count):
        for band in range(bands):
            to_band, to_lon = band + (1 if (band % 2 == 0) == first else -1), lon
            if to_band < 0 or to_band >= bands:
                to_band, to_lon = band, (lon + count // 2) % count
            pairs.append((lon * bands + band, to_lon * bands + to_band))
    return lax.ppermute(x, ("lon", "colat"), pairs)


def call(kernel, out_shapes, specs, cost=0, out=None, **more):
    return pl.pallas_call(
        kernel,
        out_shape=out_shapes,
        in_specs=specs,
        out_specs=jax.tree.map(lambda _: out or vmem(), out_shapes),
        cost_estimate=pl.CostEstimate(flops=cost, bytes_accessed=cost, transcendentals=0),
        compiler_params=pltpu.CompilerParams(vmem_limit_bytes=16 * 2**20),
        **more,
    )


def on_device(
    forward_state, adjoint_state, layer_ids, density_table, lame_table, shear_table,
    source_cells, source_wavelet, receiver_cells, receiver_residual,
):
    dims = levels, rows, cols = layer_ids.shape
    lat_cells = rows * lax.axis_size("colat")
    lon_cells = cols * lax.axis_size("lon")
    dt = COURANT * SIN_FLOOR * R_INNER * (2.0 * math.pi / lon_cells) / 1.6
    consts = ((1.0 - R_INNER) / levels, math.pi / lat_cells, dt)
    width = cols + LANES
    tiles = cols // LANES

    def shape(*dims):
        return jax.ShapeDtypeStruct(dims, F32)

    parts = forward_state, adjoint_state
    state = jnp.concatenate([x.reshape(-1, rows, cols) for x in parts]).reshape(-1, cols)
    ids = layer_ids.reshape(levels * rows, cols)

    edges = shape(pieces(19 * rows, EDGE), levels, LANES)
    near = shape(len(NEAR), levels, cols)
    far = shape(len(FAR) + S_ROWS, levels, cols)
    extents = lat_cells, lon_cells
    edge_a, edge_b, near_a, near_b, far_a, far_b = call(
        functools.partial(pack_kernel, dims),
        [edges, edges, near, near, far, far],
        [vmem()] * 2,
        cost=10**6,
    )(state, ids)
    near_b = swap_bands(near_b, False)
    near_a = swap_bands(near_a, True)
    edge_b = swap_tiles(edge_b, False)
    edge_a = swap_tiles(edge_a, True)
    far_b = swap_bands(far_b, False)
    far_a = swap_bands(far_a, True)

    ap, cv = geometry(dims, extents)
    count = max(LANES, receiver_cells.shape[0])

    def lines(x):
        x = x.astype(F32).reshape(-1, x.shape[-1])
        return jnp.pad(x, ((0, 0), (0, count - x.shape[1])))

    given = jnp.concatenate(
        [lines(x) for x in (receiver_cells, receiver_residual, source_cells, source_wavelet)]
    )
    leaving = shape(len(VEL) * tiles + side_plan()[1], levels, LANES)
    stress_shape = shape(12, rows + 2 * S_ROWS, levels, width)
    mats_shape = shape(3, rows + 2 * S_ROWS, levels, width)
    vel_shape = shape(6, rows, levels, width)
    stress, vel, rho, id_side, pay_b = call(
        functools.partial(velocity_kernel, dims, consts),
        [stress_shape, vel_shape, shape(rows, levels, width), shape(rows, levels, LANES), leaving],
        [vmem()] * 9 + [smem()],
        cost=10**7,
    )(state, ids, edge_a, edge_b, near_a, near_b, ap, cv, given, density_table)
    got_b = swap_bands(pay_b, False)
    vel, pay_a = call(
        functools.partial(rest_kernel, dims, consts), [vel_shape, leaving], [vmem()] * 6, cost=10**7
    )(stress, vel, rho, id_side, ap, cv)
    got_a = swap_bands(pay_a, True)

    first, second = call(
        functools.partial(inject_kernel, dims, extents),
        [shape(4, rows + 2 * V_ROWS, levels, width)] * 2,
        [vmem()],
        cost=10**8,
    )(given)
    halo, mats, full_vel, *inner_parts = call(
        functools.partial(fill_kernel, dims, consts),
        [
            shape(12, 2 * S_ROWS, levels, cols),
            mats_shape,
            vel_shape,
            shape(12, rows - 2 * INNER, levels, width),
            shape(6, rows - 2 * INNER - 4, levels, width),
            shape(rows - 2 * INNER - 4, levels, cols),
            shape(12, rows - 2 * INNER - 8, levels, cols),
        ],
        [vmem()] * 11 + [smem()] * 3,
        cost=10**8,
    )(
        stress, vel, ids, edge_a, edge_b, far_a, far_b, first, second, ap, cv,
        density_table, lame_table, shear_table,
    )

    flat = (9 * levels * rows, cols), (9 * levels * rows, cols), (levels * rows, cols)
    fwd, adj, density = call(
        functools.partial(final_kernel, dims, consts),
        [shape(*x) for x in flat],
        [vmem()] * 14 + [smem()] * 3,
        cost=10**8,
        out=pl.BlockSpec(memory_space=pltpu.HBM),
        scratch_shapes=[
            pltpu.VMEM((6, rows + 2 * V_ROWS, levels, width), F32),
            pltpu.VMEM(stress_shape.shape, F32),
            pltpu.VMEM(mats_shape.shape, F32),
        ]
        + [pltpu.VMEM(x, F32) for x in flat]
        + [pltpu.SemaphoreType.DMA((5,))],
    )(
        full_vel, stress, halo, got_a, got_b, mats, first, second, ap, cv,
        *inner_parts, density_table, lame_table, shear_table,
    )
    return (
        fwd.reshape(forward_state.shape),
        adj.reshape(adjoint_state.shape),
        density.reshape(layer_ids.shape),
    )


def solution(mesh):
    return jax.shard_map(
        on_device,
        mesh=mesh,
        in_specs=(
            P(None, None, "colat", "lon"),
            P(None, None, "colat", "lon"),
            P(None, "colat", "lon"),
        )
        + (P(),) * 7,
        out_specs=(
            P(None, None, "colat", "lon"),
            P(None, None, "colat", "lon"),
            P(None, "colat", "lon"),
        ),
        check_vma=False,
    )
```
